32 devices in a mesh: dp: 8 (over y, x, core), tensor: 4 (over z).
Axes of the slice: x: 2, y: 2, z: 4, core: 2. Of those that a mesh axis runs over, the one named last changes fastest.
Arguments:
- layer_input: bfloat16 [2048, 4096], P(('dp', 'tensor')), parts along dimension 0, may hold values from -6 to 10
- norm_gain: float32 [4096], replicated, may hold values from 0.25 to 1.75
- query_weight: bfloat16 [4096, 4096], P(None, 'tensor'), may hold values from -1 to 1
- key_weight: bfloat16 [4096, 1024], P(None, 'tensor'), may hold values from -1 to 1
- value_matrix: bfloat16 [4096, 1024], P(None, 'tensor'), may hold values from -0.09375 to 0.09375
- output_weight: bfloat16 [4096, 4096], P('tensor'), may hold values from -0.09375 to 0.09375
- keep_bits: int32 [256, 4, 4], P(('dp', 'tensor')), parts along dimension 0, may hold values 0 or 1
Outputs:
- layer_output: bfloat16 [2048, 4096], P(('dp', 'tensor')), parts along dimension 0
The draws below stay inside these ranges and needn't reach their ends.
There are 8 independent parts, one for each index of `dp`. The reference program is written for one: setup_inputs(seed, part) draws one part's arguments, and reference() takes and returns one part's arrays. A program takes and returns all parts, laid end to end along the dimension named above; an argument that names none is the same for every part. Nothing has to cross between parts.
All inputs are finite; a program needn't handle non-finite values. No bound on the sum of `keep_bits` on one device may be relied on, other than what follows from the above.
Results may differ from the reference program's by a relative error of at most 0.0095.
Values may be sent and summed in bfloat16 or wider, within the bound.
A program may use at most 128 MiB of HBM per device.

```python
import math
import jax
import jax.numpy as jnp
from jax import lax

MODEL_WIDTH = 4096
QUERY_HEADS = 32
KEY_VALUE_HEADS = 8
HEAD_SIZE = 128
BLOCK = 64
LEN = 256
NB = 4
N_TENSOR = 4


def draw_layer_input(key, part):
    rotary_base = jax.random.truncated_normal(jax.random.fold_in(key, 201), -6.0, 6.0, (LEN, MODEL_WIDTH), jnp.float32)
    return rotary_base.astype(jnp.bfloat16)


def draw_query_weight(key, part):
    rotary_base = jax.random.truncated_normal(jax.random.fold_in(key, 101), -4.0, 4.0, (MODEL_WIDTH, QUERY_HEADS * HEAD_SIZE), jnp.float32) / math.sqrt(MODEL_WIDTH)
    return rotary_base.astype(jnp.bfloat16)


def draw_key_weight(key, part):
    rotary_base = jax.random.truncated_normal(jax.random.fold_in(key, 102), -4.0, 4.0, (MODEL_WIDTH, KEY_VALUE_HEADS * HEAD_SIZE), jnp.float32) / math.sqrt(MODEL_WIDTH)
    return rotary_base.astype(jnp.bfloat16)


def plant(array, key, low, top_value):
    shape = array.shape
    index_at = [jax.random.randint(jax.random.fold_in(key, axis), (), 0, shape[axis]) for axis in range(len(shape))]
    array = array.at[tuple(index_at)].set(low)
    longest = shape.index(max(shape))
    index_at[longest] = (index_at[longest] + 1) % shape[longest]
    return array.at[tuple(index_at)].set(top_value)


def steps_of(stream_key, shape, cuts, smallest, largest):
    def one(position, blocks):
        steps = jax.random.uniform(jax.random.fold_in(jax.random.fold_in(stream_key, 6), position), (blocks,), jnp.float32, smallest / len(cuts), largest / len(cuts))
        return jnp.repeat(jnp.exp(steps), shape[position] // blocks).reshape((-1,) + (1,) * (len(shape) - position - 1))

    level = one(*cuts[0])
    for cut in cuts[1:]:
        level = level * one(*cut)
    return level


def gaussian(rng, dims, deviation, most, pieces=(), kind=jnp.bfloat16):
    factor_of = steps_of(rng, dims, pieces, -0.22, 0.18) if pieces else 1.0
    values = jax.random.normal(rng, dims, jnp.float32) * deviation * factor_of
    return jnp.minimum(jnp.maximum(values, -most), most).astype(kind)


def setup_inputs(seed: int = 0, part: int = 0) -> dict:
    key_of = jax.random.split(jax.random.key(seed), 8)
    part_splits = jax.random.split(jax.random.fold_in(key_of[7], part), 8)
    return {
        "layer_input": draw_layer_input(jax.random.fold_in(jax.random.fold_in(key_of[7], part), 71), part),
        "norm_gain": jnp.clip(1.0 + 0.15 * jax.random.normal(key_of[1], (MODEL_WIDTH,), jnp.float32), 0.25, 1.75),
        "query_weight": draw_query_weight(jax.random.fold_in(key_of[7], 71), part),
        "key_weight": draw_key_weight(jax.random.fold_in(key_of[7], 71), part),
        "value_matrix": gaussian(key_of[4], (MODEL_WIDTH, KEY_VALUE_HEADS * HEAD_SIZE), MODEL_WIDTH ** -0.5, 0.09375, ((1, 4),)),
        "output_weight": gaussian(key_of[5], (QUERY_HEADS * HEAD_SIZE, MODEL_WIDTH), (QUERY_HEADS * HEAD_SIZE) ** -0.5, 0.09375, ((0, 4),)),
        "keep_bits": plant((jax.random.randint(part_splits[6], (QUERY_HEADS, NB, NB), 0, 10) < 9).astype(jnp.int32), jax.random.fold_in(part_splits[6], 1), 0, 1),
    }


theta_base = 1000000.0

def apply_rotary(block, token_positions):
    half = block.shape[-1] // 2
    freqs = theta_base ** (-(jnp.arange(half, dtype=jnp.float32) * 2.0) / block.shape[-1])
    angles = token_positions[:, None] * freqs[None, :]
    cosine = jnp.cos(angles)
    sine = jnp.sin(angles)
    first = block[..., :half]
    second = block[..., half:]
    return jnp.concatenate([first * cosine - second * sine, second * cosine + first * sine], axis=-1)

def attend(query, key_rows, value_rows, keep_bits):
    heads, sequence_length, width = query.shape
    count = min(8, max(1, sequence_length // 512))
    height = sequence_length // count
    divisor = jnp.sqrt(jnp.float32(HEAD_SIZE))
    results = []
    for number in range(count):
        first_row = number * height
        last_row = first_row + height
        scores = jnp.einsum('hqd,hkd->hqk', query[:, first_row:last_row].astype(jnp.float32), key_rows[:, :last_row].astype(jnp.float32)) / divisor
        causal = jnp.arange(last_row)[None, :] <= jnp.arange(first_row, last_row)[:, None]
        scores = jnp.where(causal[None], scores, jnp.float32(-1e+30))
        highest = lax.optimization_barrier(jnp.max(scores, axis=-1, keepdims=True))
        expo_terms = jnp.exp(scores - highest)
        weights = expo_terms / lax.optimization_barrier(jnp.sum(expo_terms, axis=-1, keepdims=True))
        chosen_bits = keep_bits[:, first_row // BLOCK:last_row // BLOCK, :last_row // BLOCK].astype(jnp.float32)
        keeper = jnp.broadcast_to(chosen_bits[:, :, None, :, None], (heads, height // BLOCK, BLOCK, last_row // BLOCK, BLOCK)).reshape(heads, height, last_row)
        dropped = (weights * keeper / 0.9).astype(jnp.bfloat16)
        outcome = jnp.einsum('hqk,hkd->hqd', dropped.astype(jnp.float32), value_rows[:, :last_row].astype(jnp.float32))
        results.append(outcome.astype(jnp.bfloat16))
    return jnp.concatenate(results, axis=1)

def reference(layer_input, norm_gain, query_weight, key_weight, value_matrix, output_weight, keep_bits):
    sequence_length = layer_input.shape[0]
    inputs = layer_input.astype(jnp.float32)
    scaled = lax.rsqrt(lax.optimization_barrier(jnp.mean(inputs * inputs, axis=-1, keepdims=True)) + 1e-05)
    normed = (inputs * scaled * norm_gain[None, :]).astype(jnp.bfloat16)
    token_positions = jnp.arange(sequence_length).astype(jnp.float32)
    query_raw = jnp.dot(normed, query_weight, preferred_element_type=jnp.float32)
    key_unrotated = jnp.dot(normed, key_weight, preferred_element_type=jnp.float32).astype(jnp.bfloat16)
    value_rows = jnp.dot(normed, value_matrix, preferred_element_type=jnp.float32).astype(jnp.bfloat16)
    query = apply_rotary(query_raw.reshape(sequence_length, QUERY_HEADS, HEAD_SIZE).transpose(1, 0, 2), token_positions).astype(jnp.bfloat16)
    key_rows = apply_rotary(key_unrotated.astype(jnp.float32).reshape(sequence_length, KEY_VALUE_HEADS, HEAD_SIZE).transpose(1, 0, 2), token_positions).astype(jnp.bfloat16)
    value_rows = value_rows.reshape(sequence_length, KEY_VALUE_HEADS, HEAD_SIZE).transpose(1, 0, 2)
    query_group = QUERY_HEADS // KEY_VALUE_HEADS
    key_rows = jnp.repeat(key_rows, query_group, axis=0)
    value_rows = jnp.repeat(value_rows, query_group, axis=0)
    heads = attend(query, key_rows, value_rows, keep_bits)
    heads_out = heads.transpose(1, 0, 2).reshape(sequence_length, QUERY_HEADS * HEAD_SIZE)
    columns = QUERY_HEADS * HEAD_SIZE // N_TENSOR
    grouped = heads_out.reshape(sequence_length, N_TENSOR, columns).transpose(1, 0, 2)
    weight_rows = output_weight.reshape(N_TENSOR, columns, MODEL_WIDTH)

    def add_part(total, items):
        part_in, part_rows = items
        part = lax.optimization_barrier(jnp.dot(part_in, part_rows, preferred_element_type=jnp.float32).astype(jnp.bfloat16))
        return (total + part.astype(jnp.float32), None)
    total, unused = lax.scan(add_part, jnp.zeros((sequence_length, MODEL_WIDTH), jnp.float32), (grouped, weight_rows))
    return (inputs + total).astype(jnp.bfloat16)
```

```python
import functools

import jax
import jax.numpy as jnp
import numpy as np
from jax import lax
from jax.experimental import pallas as pl
from jax.experimental.pallas import tpu as pltpu
from jax.sharding import PartitionSpec as P

QUERY_HEADS = 32
KEY_VALUE_HEADS = 8
HEAD_SIZE = 128
BLOCK = 64


theta_base = 1000000.0


def as_sent(array):

    def short(part):
        return part.astype(jnp.bfloat16) if part.dtype == jnp.float32 else part

    return jax.tree.map(short, array)


def from_partner(array, axis, distance):
    return lax.ppermute(array, axis, [(i, i ^ 1 << distance) for i in range(lax.axis_size(axis))])


def apply_rotary(block, token_positions):
    half = block.shape[-1] // 2
    freqs = theta_base ** (-(jnp.arange(half, dtype=jnp.float32) * 2.0) / block.shape[-1])
    angles = token_positions[:, None] * freqs[None, :]
    cosine = jnp.cos(angles)
    sine = jnp.sin(angles)
    first = block[..., :half]
    second = block[..., half:]
    return jnp.concatenate(
        [first * cosine - second * sine, second * cosine + first * sine], axis=-1
    )


def join_pairs(mine, other, lowbit):
    ahead = jnp.concatenate([mine, other], axis=-1)
    behind = jnp.concatenate([other, mine], axis=-1)
    return jnp.where(lowbit, ahead, behind)


def attend(query, key_rows, value_rows, keep_bits):
    heads, sequence_length, width = query.shape
    count = min(8, max(1, sequence_length // 512))
    height = sequence_length // count
    divisor = jnp.sqrt(jnp.float32(HEAD_SIZE))
    results = []
    for number in range(count):
        first_row = number * height
        last_row = first_row + height
        scores = (
            jnp.einsum(
                "hqd,hkd->hqk",
                query[:, first_row:last_row],
                key_rows[:, :last_row],
                preferred_element_type=jnp.float32,
            )
            / divisor
        )
        causal = jnp.arange(last_row)[None, :] <= jnp.arange(first_row, last_row)[:, None]
        scores = jnp.where(causal[None], scores, jnp.float32(-1e30))
        highest = jnp.max(scores, axis=-1, keepdims=True)
        expo_terms = jnp.exp(scores - highest)
        weights = expo_terms / jnp.sum(expo_terms, axis=-1, keepdims=True)
        chosen_bits = keep_bits[
            :, first_row // BLOCK : last_row // BLOCK, : last_row // BLOCK
        ].astype(jnp.float32)
        keeper = jnp.broadcast_to(
            chosen_bits[:, :, None, :, None],
            (heads, height // BLOCK, BLOCK, last_row // BLOCK, BLOCK),
        ).reshape(heads, height, last_row)
        dropped = (weights * keeper / 0.9).astype(jnp.bfloat16)
        outcome = jnp.einsum(
            "hqk,hkd->hqd", dropped, value_rows[:, :last_row], preferred_element_type=jnp.float32
        )
        results.append(outcome.astype(jnp.bfloat16))
    return jnp.concatenate(results, axis=1)


def on_device(
    layer_input, norm_gain, query_weight, key_weight, value_matrix, output_weight, keep_bits
):
    devices = lax.axis_size("tensor")
    paired = lax.axis_size("dp") % 2 == 0
    if devices == CHAIN and paired and layer_input.shape[0] == BLOCK:
        return fused(
            layer_input,
            norm_gain,
            query_weight,
            key_weight,
            value_matrix,
            output_weight,
            keep_bits,
        )
    position = lax.axis_index("tensor")
    sharing = devices // KEY_VALUE_HEADS if devices > KEY_VALUE_HEADS else 1
    rounds = sharing.bit_length() - 1
    inputs = layer_input.astype(jnp.float32)
    scaled = lax.rsqrt(jnp.mean(inputs * inputs, axis=-1, keepdims=True) + 1e-05)
    normed = (inputs * scaled * norm_gain[None, :]).astype(jnp.bfloat16)
    query_cols = query_weight.shape[1]
    kv_cols = key_weight.shape[1]
    piece = lax.all_gather(normed, "tensor", axis=0, tiled=True)
    projected = jnp.concatenate(
        [
            jnp.dot(piece, query_weight, preferred_element_type=jnp.float32),
            jnp.dot(piece, key_weight, preferred_element_type=jnp.float32),
            jnp.dot(piece, value_matrix, preferred_element_type=jnp.float32),
        ],
        axis=1,
    )
    query_raw = projected[:, :query_cols]
    paired = jnp.stack(
        [projected[:, query_cols : query_cols + kv_cols], projected[:, query_cols + kv_cols :]]
    ).astype(jnp.bfloat16)
    for level in range(rounds):
        other = from_partner(as_sent(paired), "tensor", level).astype(paired.dtype)
        paired = join_pairs(paired, other, position >> level & 1 == 0)
    sequence_length = query_raw.shape[0]
    local_heads = query_cols // HEAD_SIZE
    local_kv = paired.shape[2] // HEAD_SIZE
    token_positions = jnp.arange(sequence_length).astype(jnp.float32)
    query = apply_rotary(
        query_raw.reshape(sequence_length, local_heads, HEAD_SIZE).transpose(1, 0, 2),
        token_positions,
    ).astype(jnp.bfloat16)
    key_rows = apply_rotary(
        paired[0]
        .astype(jnp.float32)
        .reshape(sequence_length, local_kv, HEAD_SIZE)
        .transpose(1, 0, 2),
        token_positions,
    ).astype(jnp.bfloat16)
    value_rows = paired[1].reshape(sequence_length, local_kv, HEAD_SIZE).transpose(1, 0, 2)
    query_group = QUERY_HEADS // KEY_VALUE_HEADS
    if local_heads >= query_group:
        key_rows = jnp.repeat(key_rows, query_group, axis=0)
        value_rows = jnp.repeat(value_rows, query_group, axis=0)
    else:
        key_rows = jnp.broadcast_to(key_rows, (local_heads, sequence_length, HEAD_SIZE))
        value_rows = jnp.broadcast_to(value_rows, (local_heads, sequence_length, HEAD_SIZE))
    heads = attend(query, key_rows, value_rows, keep_bits)
    heads_out = heads.transpose(1, 0, 2).reshape(sequence_length, query_cols)
    terms = jnp.dot(heads_out, output_weight, preferred_element_type=jnp.float32).astype(
        jnp.bfloat16
    )
    total = lax.psum_scatter(terms, "tensor", scatter_dimension=0, tiled=True).astype(jnp.float32)
    return (inputs + total).astype(jnp.bfloat16)


MESH = pl.DeviceIdType.MESH
CHAIN = 4
PIECES = 8
SLOT = 4
LAG = 4


def chain_kernel(
    n,
    x_hbm,
    gain_hbm,
    keep_hbm,
    cos_hbm,
    sin_hbm,
    wq_hbm,
    wk_hbm,
    wv_hbm,
    wo_hbm,
    out_ref,
    x_ref,
    gain_ref,
    keep_ref,
    cos_ref,
    sin_ref,
    wq,
    wk,
    wv,
    wo,
    gathered,
    parts,
    incoming,
    keys,
    values,
    queries,
    joined,
    projected,
    load_sem,
    ag_send,
    ag_recv,
    rs_send,
    rs_recv,
    turn,
):
    me = lax.axis_index("tensor")
    rows, width = x_ref.shape
    length = n * rows
    step = width // PIECES
    heads = wq.shape[1] // HEAD_SIZE
    kv_heads = wk.shape[1] // HEAD_SIZE
    group = heads // kv_heads
    blocks = keep_ref.shape[1]
    has_left = me > 0
    has_right = me < n - 1
    is_lower = me < n // 2
    is_end = jnp.logical_or(me == 0, me == n - 1)
    pair = lax.axis_index("dp")
    leads = lax.rem(pair, 2) == 0
    partner = jnp.where(leads, pair + 1, pair - 1)

    loads = [
        pltpu.make_async_copy(src, dst, load_sem.at[i])
        for i, (src, dst) in enumerate(
            (
                (x_hbm, x_ref),
                (gain_hbm, gain_ref),
                (keep_hbm, keep_ref),
                (wk_hbm, wk),
                (wv_hbm, wv),
                (wq_hbm, wq),
                (cos_hbm, cos_ref),
                (sin_hbm, sin_ref),
                (wo_hbm, wo),
            )
        )
    ]

    barrier = pltpu.get_barrier_semaphore()

    @pl.when(has_left)
    def _():
        pl.semaphore_signal(barrier, inc=1, device_id={"tensor": me - 1}, device_id_type=MESH)

    @pl.when(has_right)
    def _():
        pl.semaphore_signal(barrier, inc=1, device_id={"tensor": me + 1}, device_id_type=MESH)

    pl.semaphore_signal(barrier, inc=1, device_id={"dp": partner}, device_id_type=MESH)

    for load in loads[:3]:
        load.start()
    loads[0].wait()
    loads[1].wait()
    for load in loads[3:]:
        load.start()

    def slot(device, block):
        return lax.rem(block + jnp.where(device == 2, 2, 0), n)

    inputs = x_ref[...].astype(jnp.float32)
    scaled = lax.rsqrt(jnp.mean(inputs * inputs, axis=-1, keepdims=True) + 1e-05)
    gathered[slot(me, me)] = (inputs * scaled * gain_ref[...]).astype(jnp.bfloat16)

    pl.semaphore_wait(barrier, jnp.where(is_end, 2, 3))

    def cols(c):
        return pl.ds(pl.multiple_of(c * step, step), step)

    def gather_copy(way, block, c):
        to = me + 1 - 2 * way
        return pltpu.make_async_remote_copy(
            src_ref=gathered.at[slot(me, block), :, cols(c)],
            dst_ref=gathered.at[slot(to, block), :, cols(c)],
            send_sem=ag_send.at[way, block],
            recv_sem=ag_recv.at[block, c],
            device_id={"tensor": to},
            device_id_type=MESH,
        )

    def arrived(block, c):
        arrival(block, c)

    def arrival(block, c):
        piece = gathered.at[slot(me, block), :, cols(c)]
        pltpu.make_async_remote_copy(
            src_ref=piece,
            dst_ref=piece,
            send_sem=ag_send.at[0, 0],
            recv_sem=ag_recv.at[block, c],
            device_id={"tensor": jnp.where(has_right, me + 1, me - 1)},
            device_id_type=MESH,
        ).wait_recv()

    def sum_copy(way, token, c):
        return pltpu.make_async_remote_copy(
            src_ref=parts.at[token, :, cols(c)],
            dst_ref=incoming.at[way, token, :, cols(c)],
            send_sem=rs_send.at[token],
            recv_sem=rs_recv.at[way, token, c],
            device_id={"tensor": me + 1 - 2 * way},
            device_id_type=MESH,
        )

    def whole_copy(buffer, sem, index):
        return pltpu.make_async_remote_copy(
            src_ref=buffer.at[index],
            dst_ref=buffer.at[index],
            send_sem=sem,
            recv_sem=ag_recv.at[0, 0],
            device_id={"tensor": jnp.where(has_right, me + 1, me - 1)},
            device_id_type=MESH,
        )

    def each(first, last, body):
        lax.fori_loop(first, last, lambda c, carry: (body(c), carry)[1], 0)

    early = jnp.where(me == 0, PIECES, jnp.where(leads, me * PIECES // 2, 0))

    def send_own():
        @pl.when(has_right)
        def _():
            each(0, early, lambda c: gather_copy(0, me, c).start())

        @pl.when(has_left)
        def _():
            each(0, PIECES, lambda c: gather_copy(1, me, c).start())

    pl.when(leads)(send_own)

    def take_turn():
        @pl.when(jnp.logical_not(leads))
        def _():
            pl.semaphore_wait(turn, 1)
            send_own()

    def give_turn():
        pl.semaphore_signal(turn, inc=1, device_id={"dp": partner}, device_id_type=MESH)

    def rest_of_own():
        each(early, PIECES, lambda c: gather_copy(0, me, c).start())

    def forward(way, block, c):
        arrived(block, c)
        gather_copy(way, block, c).start()

    def rotated(t, cosine, sine):
        return t * cosine + pltpu.roll(t, HEAD_SIZE // 2, 1) * sine

    def multiply(first, count, where):
        block = gathered[pl.ds(first, count), :, where].reshape(count * rows, -1)
        spans = []
        at = 0
        for weight in (wq, wk, wv):
            product = jnp.dot(block, weight[where, :], preferred_element_type=jnp.float32)
            spans.append((slice(at, at + weight.shape[1]), product.reshape(count, rows, -1)))
            at += weight.shape[1]
        return spans

    def multiply_whole(first):
        for span, product in multiply(first, 1, slice(None)):
            projected[pl.ds(first, 1), :, span] = product

    def multiply_piece(first, count, c):
        for span, product in multiply(first, count, cols(c)):
            projected[pl.ds(first, count), :, span] += product

    def attend_block(token):
        here = slot(me, token)
        first_row = pl.multiple_of(token * rows, rows)
        where = pl.ds(first_row, rows)
        q_cols, kv_cols = wq.shape[1], wk.shape[1]
        cosine = cos_ref[where, :]
        sine = sin_ref[where, :]
        key_raw = (
            projected[here, :, q_cols : q_cols + kv_cols].astype(jnp.bfloat16).astype(jnp.float32)
        )
        value = projected[here, :, q_cols + kv_cols :].astype(jnp.bfloat16)
        for g in range(kv_heads):
            span = slice(g * HEAD_SIZE, (g + 1) * HEAD_SIZE)
            keys[g, where, :] = rotated(key_raw[:, span], cosine, sine).astype(jnp.bfloat16)
            values[g, where, :] = value[:, span]
        for g in range(kv_heads):
            wide = slice(g * group * HEAD_SIZE, (g + 1) * group * HEAD_SIZE)
            raw = projected[here, :, wide]
            for h in range(group):
                one = raw[:, h * HEAD_SIZE : (h + 1) * HEAD_SIZE]
                queries[g, h * rows : (h + 1) * rows, :] = rotated(one, cosine, sine).astype(
                    jnp.bfloat16
                )
        column = lax.broadcasted_iota(jnp.int32, (rows, length), 1)
        row = lax.broadcasted_iota(jnp.int32, (rows, length), 0) + first_row
        causal = column <= row
        which = lax.broadcasted_iota(jnp.int32, (1, length), 1) // (length // blocks)
        for g in range(kv_heads):
            scores = lax.dot_general(
                queries[g], keys[g], (((1,), (1,)), ((), ())), preferred_element_type=jnp.float32
            ) * np.float32(1.0 / np.sqrt(HEAD_SIZE))
            dropped = []
            for h in range(group):
                one = jnp.where(causal, scores[h * rows : (h + 1) * rows], jnp.float32(-1e30))
                highest = jnp.max(one, axis=-1, keepdims=True)
                terms = jnp.exp(one - highest)
                inverse = 1.0 / (jnp.sum(terms, axis=-1, keepdims=True) * jnp.float32(0.9))
                keeper = jnp.zeros((1, length), jnp.float32)
                for j in range(blocks):
                    bit = keep_ref[token, j, g * group + h].astype(jnp.float32)
                    keeper = jnp.where(which == j, bit, keeper)
                dropped.append((terms * inverse * keeper).astype(jnp.bfloat16))
            result = jnp.dot(
                jnp.concatenate(dropped, axis=0), values[g], preferred_element_type=jnp.float32
            ).astype(jnp.bfloat16)
            for h in range(group):
                at = (g * group + h) * HEAD_SIZE
                joined[token, :, at : at + HEAD_SIZE] = result[h * rows : (h + 1) * rows]

    def project(first, count, c):
        mixed = joined[pl.ds(first, count)].reshape(count * rows, -1)
        parts[pl.ds(first, count), :, cols(c)] = (
            jnp.dot(mixed, wo[:, cols(c)], preferred_element_type=jnp.float32)
            .astype(jnp.bfloat16)
            .reshape(count, rows, -1)
        )

    def pass_on(token, c):
        way = jnp.where(me < token, 0, 1)
        sum_copy(way, token, c).wait_recv()
        total = parts[token, :, cols(c)].astype(jnp.float32) + incoming[
            way, token, :, cols(c)
        ].astype(jnp.float32)
        parts[token, :, cols(c)] = total.astype(jnp.bfloat16)
        sum_copy(way, token, c).start()

    keys[...] = jnp.zeros_like(keys)
    values[...] = jnp.zeros_like(values)
    projected[...] = jnp.zeros_like(projected)
    for load in loads[3:6]:
        load.wait()

    def wait_tables():
        for load in loads[6:] + loads[2:3]:
            load.wait()

    def drain_gather(early_up, early_down):
        def drain(block):
            @pl.when(functools.reduce(jnp.logical_and, (block <= me, has_right, block >= early_up)))
            def _():
                sent(0, block)

            @pl.when(functools.reduce(jnp.logical_and, (block >= me, has_left, block >= early_down)))
            def _():
                sent(1, block)

        each(0, n, drain)

    def sent(way, block):
        whole_copy(gathered, ag_send.at[way, block], block).wait_send()

    @pl.when(is_end)
    def _():
        way = jnp.where(me == 0, 0, 1)
        multiply_whole(me)
        wait_tables()

        @pl.when(jnp.logical_and(leads, me > 0))
        def _():
            sent(1, me)
            give_turn()

        take_turn()

        def iteration(i, carry):
            @pl.when(i != me)
            def _():
                def piece(c):
                    arrived(i, c)
                    multiply_piece(i, 1, c)

                each(0, PIECES, piece)

            attend_block(i)

            @pl.when(functools.reduce(jnp.logical_and, (i == 0, me == 0, leads)))
            def _():
                sent(0, 0)
                give_turn()

            def out_piece(c):
                project(i, 1, c)

                @pl.when(i != me)
                def _():
                    sum_copy(way, i, c).start()

            each(0, PIECES, out_piece)
            return carry

        lax.fori_loop(0, n, iteration, 0)

        drain_gather(jnp.where(leads, n, 0), jnp.where(leads, n, 0))

        def finish(c):
            sum_copy(1 - way, me, c).wait_recv()
            out_ref[:, cols(c)] = (
                x_ref[:, cols(c)].astype(jnp.float32)
                + parts[me, :, cols(c)].astype(jnp.float32)
                + incoming[1 - way, me, :, cols(c)].astype(jnp.float32)
            ).astype(out_ref.dtype)

        each(0, PIECES, finish)

    @pl.when(jnp.logical_not(is_end))
    def _():
        last = jnp.where(is_lower, n - 1, 1)
        last_way = jnp.where(is_lower, 1, 0)
        skew = (me - 1) * 2
        split = jnp.where(is_lower, n - 1, 1)
        take_turn()

        def multiply_last(c):
            multiply_piece(3, 1, c)

        def attend(i):
            attend_block(i)

        def both(c):
            @pl.when(c < PIECES)
            def _():
                forward(1, me + 1, c)

            @pl.when(c >= skew)
            def _():
                forward(0, 0, c - skew)
                multiply_piece(0, 3, c - skew)

        each(0, PIECES + skew, both)
        wait_tables()

        @pl.when(is_lower)
        def _():
            rest_of_own()

        @pl.when(leads)
        def _():
            sent(1, me)
            sent(1, me + 1)
            give_turn()

        each(0, split, attend)

        @pl.when(is_lower)
        def _():
            def out_piece(c):
                project(0, 3, c)
                forward(last_way, last, c)

            each(0, PIECES, out_piece)

        @pl.when(jnp.logical_not(is_lower))
        def _():
            def out_piece(c):
                project(0, 1, c)
                forward(last_way, last, c)

            each(0, PIECES, out_piece)
            rest_of_own()

        each(0, PIECES, lambda c: multiply_last(c))
        each(split, n, attend)

        @pl.when(is_lower)
        def _():
            each(0, PIECES, lambda c: project(n - 1, 1, c))

            def stream(k):
                token = 2 + k // PIECES
                pass_on(token, lax.rem(k, PIECES))

                @pl.when(jnp.logical_and(k >= LAG, k < PIECES + LAG))
                def _():
                    pass_on(0, k - LAG)

            each(0, 2 * PIECES, stream)

        @pl.when(jnp.logical_not(is_lower))
        def _():
            def out_piece(c):
                project(1, 3, c)
                pass_on(0, c)

            each(0, PIECES, out_piece)

            def two(c):
                @pl.when(c < PIECES)
                def _():
                    pass_on(1, c)

                @pl.when(c >= LAG)
                def _():
                    pass_on(n - 1, c - LAG)

            each(0, PIECES + LAG, two)

        drain_gather(0, jnp.where(leads, me + 2, 0))

        def finish(c):
            for way in range(2):
                sum_copy(way, me, c).wait_recv()
            out_ref[:, cols(c)] = (
                x_ref[:, cols(c)].astype(jnp.float32)
                + parts[me, :, cols(c)].astype(jnp.float32)
                + incoming[0, me, :, cols(c)].astype(jnp.float32)
                + incoming[1, me, :, cols(c)].astype(jnp.float32)
            ).astype(out_ref.dtype)

        each(0, PIECES, finish)

    def drain(token):
        @pl.when(token != me)
        def _():
            whole_copy(parts, rs_send.at[token], token).wait_send()

    each(0, n, drain)


def fused(layer_input, norm_gain, query_weight, key_weight, value_matrix, output_weight, keep_bits):
    n = lax.axis_size("tensor")
    rows, width = layer_input.shape
    length = n * rows
    half = HEAD_SIZE // 2
    freqs = theta_base ** (-(np.arange(half, dtype=np.float64) * 2.0) / HEAD_SIZE)
    angles = np.arange(length)[:, None] * freqs[None, :]
    cosine = np.concatenate([np.cos(angles), np.cos(angles)], axis=1).astype(np.float32)
    sine = np.concatenate([-np.sin(angles), np.sin(angles)], axis=1).astype(np.float32)
    heads = query_weight.shape[1] // HEAD_SIZE
    kv_heads = key_weight.shape[1] // HEAD_SIZE
    vmem = pl.BlockSpec(memory_space=pltpu.VMEM)
    hbm = pl.BlockSpec(memory_space=pltpu.HBM)
    bf16 = jnp.bfloat16
    weights = (query_weight, key_weight, value_matrix, output_weight)
    return pl.pallas_call(
        functools.partial(chain_kernel, n),
        out_shape=jax.ShapeDtypeStruct((rows, width), bf16),
        in_specs=[hbm] * 9,
        out_specs=vmem,
        scratch_shapes=[
            pltpu.VMEM((rows, width), bf16),
            pltpu.VMEM((1, width), jnp.float32),
            pltpu.SMEM(keep_bits.shape[1:] + keep_bits.shape[:1], jnp.int32),
            pltpu.VMEM(cosine.shape, jnp.float32),
            pltpu.VMEM(sine.shape, jnp.float32),
        ]
        + [pltpu.VMEM(w.shape, bf16) for w in weights]
        + [
            pltpu.VMEM((n, rows, width), bf16),
            pltpu.VMEM((n, rows, width), bf16),
            pltpu.VMEM((2, n, rows, width), bf16),
            pltpu.VMEM((kv_heads, length, HEAD_SIZE), bf16),
            pltpu.VMEM((kv_heads, length, HEAD_SIZE), bf16),
            pltpu.VMEM((kv_heads, heads // kv_heads * rows, HEAD_SIZE), bf16),
            pltpu.VMEM((n, rows, heads * HEAD_SIZE), bf16),
            pltpu.VMEM((n, rows, (heads + 2 * kv_heads) * HEAD_SIZE), jnp.float32),
            pltpu.SemaphoreType.DMA((9,)),
            pltpu.SemaphoreType.DMA((2, n)),
            pltpu.SemaphoreType.DMA((n, PIECES)),
            pltpu.SemaphoreType.DMA((n,)),
            pltpu.SemaphoreType.DMA((2, n, PIECES)),
            pltpu.SemaphoreType.REGULAR,
        ],
        compiler_params=pltpu.CompilerParams(
            collective_id=0, has_side_effects=True, vmem_limit_bytes=60 * 2**20
        ),
    )(layer_input, norm_gain[None, :], keep_bits.transpose(1, 2, 0), cosine, sine, *weights)


def solution(mesh):
    in_specs = (
        P(("dp", "tensor"), None),
        P(),
        P(None, "tensor"),
        P(None, "tensor"),
        P(None, "tensor"),
        P("tensor", None),
        P(("dp", "tensor"), None, None),
    )
    out_specs = P(("dp", "tensor"), None)
    return jax.shard_map(
        on_device, mesh=mesh, in_specs=in_specs, out_specs=out_specs, check_vma=False
    )
```

```python
import functools

import jax
import jax.numpy as jnp
import numpy as np
from jax import lax
from jax.experimental import pallas as pl
from jax.experimental.pallas import tpu as pltpu
from jax.sharding import PartitionSpec as P

QUERY_HEADS = 32
KEY_VALUE_HEADS = 8
HEAD_SIZE = 128
BLOCK = 64


theta_base = 1000000.0


def as_sent(array):

    def short(part):
        return part.astype(jnp.bfloat16) if part.dtype == jnp.float32 else part

    return jax.tree.map(short, array)


def from_partner(array, axis, distance):
    return lax.ppermute(array, axis, [(i, i ^ 1 << distance) for i in range(lax.axis_size(axis))])


def apply_rotary(block, token_positions):
    half = block.shape[-1] // 2
    freqs = theta_base ** (-(jnp.arange(half, dtype=jnp.float32) * 2.0) / block.shape[-1])
    angles = token_positions[:, None] * freqs[None, :]
    cosine = jnp.cos(angles)
    sine = jnp.sin(angles)
    first = block[..., :half]
    second = block[..., half:]
    return jnp.concatenate(
        [first * cosine - second * sine, second * cosine + first * sine], axis=-1
    )


def join_pairs(mine, other, lowbit):
    ahead = jnp.concatenate([mine, other], axis=-1)
    behind = jnp.concatenate([other, mine], axis=-1)
    return jnp.where(lowbit, ahead, behind)


def attend(query, key_rows, value_rows, keep_bits):
    heads, sequence_length, width = query.shape
    count = min(8, max(1, sequence_length // 512))
    height = sequence_length // count
    divisor = jnp.sqrt(jnp.float32(HEAD_SIZE))
    results = []
    for number in range(count):
        first_row = number * height
        last_row = first_row + height
        scores = (
            jnp.einsum(
                "hqd,hkd->hqk",
                query[:, first_row:last_row],
                key_rows[:, :last_row],
                preferred_element_type=jnp.float32,
            )
            / divisor
        )
        causal = jnp.arange(last_row)[None, :] <= jnp.arange(first_row, last_row)[:, None]
        scores = jnp.where(causal[None], scores, jnp.float32(-1e30))
        highest = jnp.max(scores, axis=-1, keepdims=True)
        expo_terms = jnp.exp(scores - highest)
        weights = expo_terms / jnp.sum(expo_terms, axis=-1, keepdims=True)
        chosen_bits = keep_bits[
            :, first_row // BLOCK : last_row // BLOCK, : last_row // BLOCK
        ].astype(jnp.float32)
        keeper = jnp.broadcast_to(
            chosen_bits[:, :, None, :, None],
            (heads, height // BLOCK, BLOCK, last_row // BLOCK, BLOCK),
        ).reshape(heads, height, last_row)
        dropped = (weights * keeper / 0.9).astype(jnp.bfloat16)
        outcome = jnp.einsum(
            "hqk,hkd->hqd", dropped, value_rows[:, :last_row], preferred_element_type=jnp.float32
        )
        results.append(outcome.astype(jnp.bfloat16))
    return jnp.concatenate(results, axis=1)


def on_device(
    layer_input, norm_gain, query_weight, key_weight, value_matrix, output_weight, keep_bits
):
    devices = lax.axis_size("tensor")
    paired = lax.axis_size("dp") % 2 == 0
    if devices == CHAIN and paired and layer_input.shape[0] == BLOCK:
        return fused(
            layer_input,
            norm_gain,
            query_weight,
            key_weight,
            value_matrix,
            output_weight,
            keep_bits,
        )
    position = lax.axis_index("tensor")
    sharing = devices // KEY_VALUE_HEADS if devices > KEY_VALUE_HEADS else 1
    rounds = sharing.bit_length() - 1
    inputs = layer_input.astype(jnp.float32)
    scaled = lax.rsqrt(jnp.mean(inputs * inputs, axis=-1, keepdims=True) + 1e-05)
    normed = (inputs * scaled * norm_gain[None, :]).astype(jnp.bfloat16)
    query_cols = query_weight.shape[1]
    kv_cols = key_weight.shape[1]
    piece = lax.all_gather(normed, "tensor", axis=0, tiled=True)
    projected = jnp.concatenate(
        [
            jnp.dot(piece, query_weight, preferred_element_type=jnp.float32),
            jnp.dot(piece, key_weight, preferred_element_type=jnp.float32),
            jnp.dot(piece, value_matrix, preferred_element_type=jnp.float32),
        ],
        axis=1,
    )
    query_raw = projected[:, :query_cols]
    paired = jnp.stack(
        [projected[:, query_cols : query_cols + kv_cols], projected[:, query_cols + kv_cols :]]
    ).astype(jnp.bfloat16)
    for level in range(rounds):
        other = from_partner(as_sent(paired), "tensor", level).astype(paired.dtype)
        paired = join_pairs(paired, other, position >> level & 1 == 0)
    sequence_length = query_raw.shape[0]
    local_heads = query_cols // HEAD_SIZE
    local_kv = paired.shape[2] // HEAD_SIZE
    token_positions = jnp.arange(sequence_length).astype(jnp.float32)
    query = apply_rotary(
        query_raw.reshape(sequence_length, local_heads, HEAD_SIZE).transpose(1, 0, 2),
        token_positions,
    ).astype(jnp.bfloat16)
    key_rows = apply_rotary(
        paired[0]
        .astype(jnp.float32)
        .reshape(sequence_length, local_kv, HEAD_SIZE)
        .transpose(1, 0, 2),
        token_positions,
    ).astype(jnp.bfloat16)
    value_rows = paired[1].reshape(sequence_length, local_kv, HEAD_SIZE).transpose(1, 0, 2)
    query_group = QUERY_HEADS // KEY_VALUE_HEADS
    if local_heads >= query_group:
        key_rows = jnp.repeat(key_rows, query_group, axis=0)
        value_rows = jnp.repeat(value_rows, query_group, axis=0)
    else:
        key_rows = jnp.broadcast_to(key_rows, (local_heads, sequence_length, HEAD_SIZE))
        value_rows = jnp.broadcast_to(value_rows, (local_heads, sequence_length, HEAD_SIZE))
    heads = attend(query, key_rows, value_rows, keep_bits)
    heads_out = heads.transpose(1, 0, 2).reshape(sequence_length, query_cols)
    terms = jnp.dot(heads_out, output_weight, preferred_element_type=jnp.float32).astype(
        jnp.bfloat16
    )
    total = lax.psum_scatter(terms, "tensor", scatter_dimension=0, tiled=True).astype(jnp.float32)
    return (inputs + total).astype(jnp.bfloat16)


MESH = pl.DeviceIdType.MESH
CHAIN = 4
PIECES = 8
SLOT = 4
LAG = 4
LATE = 16


def chain_kernel(
    n,
    x_hbm,
    gain_hbm,
    keep_hbm,
    cos_hbm,
    sin_hbm,
    wq_hbm,
    wk_hbm,
    wv_hbm,
    wo_hbm,
    out_ref,
    x_ref,
    gain_ref,
    keep_ref,
    cos_ref,
    sin_ref,
    wq,
    wk,
    wv,
    wo,
    gathered,
    parts,
    incoming,
    keys,
    values,
    queries,
    joined,
    projected,
    load_sem,
    ag_send,
    ag_recv,
    rs_send,
    rs_recv,
    turn,
):
    me = lax.axis_index("tensor")
    rows, width = x_ref.shape
    length = n * rows
    step = width // PIECES
    heads = wq.shape[1] // HEAD_SIZE
    kv_heads = wk.shape[1] // HEAD_SIZE
    group = heads // kv_heads
    blocks = keep_ref.shape[1]
    has_left = me > 0
    has_right = me < n - 1
    is_lower = me < n // 2
    is_end = jnp.logical_or(me == 0, me == n - 1)
    pair = lax.axis_index("dp")
    leads = lax.rem(pair, 2) == 0
    partner = jnp.where(leads, pair + 1, pair - 1)

    loads = [
        pltpu.make_async_copy(src, dst, load_sem.at[i])
        for i, (src, dst) in enumerate(
            (
                (x_hbm, x_ref),
                (gain_hbm, gain_ref),
                (keep_hbm, keep_ref),
                (wk_hbm, wk),
                (wv_hbm, wv),
                (wq_hbm, wq),
                (cos_hbm, cos_ref),
                (sin_hbm, sin_ref),
                (wo_hbm, wo),
            )
        )
    ]

    barrier = pltpu.get_barrier_semaphore()

    @pl.when(has_left)
    def _():
        pl.semaphore_signal(barrier, inc=1, device_id={"tensor": me - 1}, device_id_type=MESH)

    @pl.when(has_right)
    def _():
        pl.semaphore_signal(barrier, inc=1, device_id={"tensor": me + 1}, device_id_type=MESH)

    pl.semaphore_signal(barrier, inc=1, device_id={"dp": partner}, device_id_type=MESH)

    for load in loads[:3]:
        load.start()
    loads[0].wait()
    loads[1].wait()
    for load in loads[3:]:
        load.start()

    def slot(device, block):
        return lax.rem(block + jnp.where(device == 2, 2, 0), n)

    inputs = x_ref[...].astype(jnp.float32)
    scaled = lax.rsqrt(jnp.mean(inputs * inputs, axis=-1, keepdims=True) + 1e-05)
    gathered[slot(me, me)] = (inputs * scaled * gain_ref[...]).astype(jnp.bfloat16)

    pl.semaphore_wait(barrier, jnp.where(is_end, 2, 3))

    def cols(c):
        return pl.ds(pl.multiple_of(c * step, step), step)

    def pairs(k):
        return pl.ds(pl.multiple_of(k * 2 * step, 2 * step), 2 * step)

    def gather_copy(way, block, c):
        to = me + 1 - 2 * way
        return pltpu.make_async_remote_copy(
            src_ref=gathered.at[slot(me, block), :, cols(c)],
            dst_ref=gathered.at[slot(to, block), :, cols(c)],
            send_sem=ag_send.at[way, block],
            recv_sem=ag_recv.at[block, c],
            device_id={"tensor": to},
            device_id_type=MESH,
        )

    def arrived(block, c):
        arrival(block, c)

    def arrival(block, c):
        piece = gathered.at[slot(me, block), :, cols(c)]
        pltpu.make_async_remote_copy(
            src_ref=piece,
            dst_ref=piece,
            send_sem=ag_send.at[0, 0],
            recv_sem=ag_recv.at[block, c],
            device_id={"tensor": jnp.where(has_right, me + 1, me - 1)},
            device_id_type=MESH,
        ).wait_recv()

    def sum_copy(way, token, c):
        return pltpu.make_async_remote_copy(
            src_ref=parts.at[token, :, cols(c)],
            dst_ref=incoming.at[way, token, :, cols(c)],
            send_sem=rs_send.at[token],
            recv_sem=rs_recv.at[way, token, c],
            device_id={"tensor": me + 1 - 2 * way},
            device_id_type=MESH,
        )

    def whole_copy(buffer, sem, index):
        return pltpu.make_async_remote_copy(
            src_ref=buffer.at[index],
            dst_ref=buffer.at[index],
            send_sem=sem,
            recv_sem=ag_recv.at[0, 0],
            device_id={"tensor": jnp.where(has_right, me + 1, me - 1)},
            device_id_type=MESH,
        )

    def each(first, last, body):
        lax.fori_loop(first, last, lambda c, carry: (body(c), carry)[1], 0)

    early = jnp.where(me == 0, PIECES, jnp.where(leads, me * PIECES // 2, 0))

    def send_own():
        @pl.when(has_right)
        def _():
            each(0, early, lambda c: gather_copy(0, me, c).start())

        @pl.when(has_left)
        def _():
            each(0, PIECES, lambda c: gather_copy(1, me, c).start())

    pl.when(leads)(send_own)

    def take_turn():
        @pl.when(jnp.logical_not(leads))
        def _():
            pl.semaphore_wait(turn, 1)
            send_own()

    def give_turn():
        pl.semaphore_signal(turn, inc=1, device_id={"dp": partner}, device_id_type=MESH)

    def rest_of_own():
        each(early, PIECES, lambda c: gather_copy(0, me, c).start())

    def forward(way, block, c):
        arrived(block, c)
        gather_copy(way, block, c).start()

    def rotated(t, cosine, sine):
        return t * cosine + pltpu.roll(t, HEAD_SIZE // 2, 1) * sine

    def multiply(first, count, where):
        block = gathered[pl.ds(first, count), :, where].reshape(count * rows, -1)
        spans = []
        at = 0
        for weight in (wq, wk, wv):
            product = jnp.dot(block, weight[where, :], preferred_element_type=jnp.float32)
            spans.append((slice(at, at + weight.shape[1]), product.reshape(count, rows, -1)))
            at += weight.shape[1]
        return spans

    def multiply_whole(first):
        for span, product in multiply(first, 1, slice(None)):
            projected[pl.ds(first, 1), :, span] = product

    def multiply_piece(first, count, where):
        for span, product in multiply(first, count, where):
            projected[pl.ds(first, count), :, span] += product

    def attend_block(token):
        here = slot(me, token)
        first_row = pl.multiple_of(token * rows, rows)
        where = pl.ds(first_row, rows)
        q_cols, kv_cols = wq.shape[1], wk.shape[1]
        cosine = cos_ref[where, :]
        sine = sin_ref[where, :]
        key_raw = (
            projected[here, :, q_cols : q_cols + kv_cols].astype(jnp.bfloat16).astype(jnp.float32)
        )
        value = projected[here, :, q_cols + kv_cols :].astype(jnp.bfloat16)
        for g in range(kv_heads):
            span = slice(g * HEAD_SIZE, (g + 1) * HEAD_SIZE)
            keys[g, where, :] = rotated(key_raw[:, span], cosine, sine).astype(jnp.bfloat16)
            values[g, where, :] = value[:, span]
        for g in range(kv_heads):
            wide = slice(g * group * HEAD_SIZE, (g + 1) * group * HEAD_SIZE)
            raw = projected[here, :, wide]
            for h in range(group):
                one = raw[:, h * HEAD_SIZE : (h + 1) * HEAD_SIZE]
                queries[g, h * rows : (h + 1) * rows, :] = rotated(one, cosine, sine).astype(
                    jnp.bfloat16
                )
        column = lax.broadcasted_iota(jnp.int32, (rows, length), 1)
        row = lax.broadcasted_iota(jnp.int32, (rows, length), 0) + first_row
        causal = column <= row
        which = lax.broadcasted_iota(jnp.int32, (1, length), 1) // (length // blocks)
        for g in range(kv_heads):
            scores = lax.dot_general(
                queries[g], keys[g], (((1,), (1,)), ((), ())), preferred_element_type=jnp.float32
            ) * np.float32(1.0 / np.sqrt(HEAD_SIZE))
            dropped = []
            for h in range(group):
                one = jnp.where(causal, scores[h * rows : (h + 1) * rows], jnp.float32(-1e30))
                highest = jnp.max(one, axis=-1, keepdims=True)
                terms = jnp.exp(one - highest)
                inverse = 1.0 / (jnp.sum(terms, axis=-1, keepdims=True) * jnp.float32(0.9))
                keeper = jnp.zeros((1, length), jnp.float32)
                for j in range(blocks):
                    bit = keep_ref[token, j, g * group + h].astype(jnp.float32)
                    keeper = jnp.where(which == j, bit, keeper)
                dropped.append((terms * inverse * keeper).astype(jnp.bfloat16))
            result = jnp.dot(
                jnp.concatenate(dropped, axis=0), values[g], preferred_element_type=jnp.float32
            ).astype(jnp.bfloat16)
            for h in range(group):
                at = (g * group + h) * HEAD_SIZE
                joined[token, :, at : at + HEAD_SIZE] = result[h * rows : (h + 1) * rows]

    def project(first, count, where):
        mixed = joined[pl.ds(first, count)].reshape(count * rows, -1)
        parts[pl.ds(first, count), :, where] = (
            jnp.dot(mixed, wo[:, where], preferred_element_type=jnp.float32)
            .astype(jnp.bfloat16)
            .reshape(count, rows, -1)
        )

    def pass_on(token, c):
        way = jnp.where(me < token, 0, 1)
        sum_copy(way, token, c).wait_recv()
        total = parts[token, :, cols(c)].astype(jnp.float32) + incoming[
            way, token, :, cols(c)
        ].astype(jnp.float32)
        parts[token, :, cols(c)] = total.astype(jnp.bfloat16)
        sum_copy(way, token, c).start()

    keys[...] = jnp.zeros_like(keys)
    values[...] = jnp.zeros_like(values)
    projected[...] = jnp.zeros_like(projected)
    for load in loads[3:6]:
        load.wait()

    def wait_tables():
        for load in loads[6:] + loads[2:3]:
            load.wait()

    def drain_gather(early_up, early_down):
        def drain(block):
            @pl.when(functools.reduce(jnp.logical_and, (block <= me, has_right, block >= early_up)))
            def _():
                sent(0, block)

            @pl.when(functools.reduce(jnp.logical_and, (block >= me, has_left, block >= early_down)))
            def _():
                sent(1, block)

        each(0, n, drain)

    def sent(way, block):
        whole_copy(gathered, ag_send.at[way, block], block).wait_send()

    @pl.when(is_end)
    def _():
        way = jnp.where(me == 0, 0, 1)
        multiply_whole(me)
        wait_tables()

        @pl.when(jnp.logical_and(leads, me > 0))
        def _():
            sent(1, me)
            give_turn()

        take_turn()
        ahead = jnp.where(jnp.logical_and(leads, me > 0), n - 2, -1)

        def stream(i):
            def piece(k):
                arrived(i, 2 * k)
                arrived(i, 2 * k + 1)
                multiply_piece(i, 1, pairs(k))

            each(0, PIECES // 2, piece)

        @pl.when(ahead >= 0)
        def _():
            stream(ahead)

        def iteration(i, carry):
            @pl.when(jnp.logical_and(i != me, i != ahead))
            def _():
                stream(i)

            attend_block(i)

            @pl.when(functools.reduce(jnp.logical_and, (i == 0, me == 0, leads)))
            def _():
                sent(0, 0)
                give_turn()

            def out_piece(k):
                project(i, 1, pairs(k))
                sum_copy(way, i, 2 * k).start()
                sum_copy(way, i, 2 * k + 1).start()

            @pl.when(i != me)
            def _():
                each(0, PIECES // 2, out_piece)

            return carry

        lax.fori_loop(0, n, iteration, 0)

        def out_own(k):
            project(me, 1, pairs(k))

        each(0, PIECES // 2, out_own)
        drain_gather(jnp.where(leads, n, 0), jnp.where(leads, n, 0))

        def finish(c):
            sum_copy(1 - way, me, c).wait_recv()
            out_ref[:, cols(c)] = (
                x_ref[:, cols(c)].astype(jnp.float32)
                + parts[me, :, cols(c)].astype(jnp.float32)
                + incoming[1 - way, me, :, cols(c)].astype(jnp.float32)
            ).astype(out_ref.dtype)

        each(0, PIECES, finish)

    @pl.when(jnp.logical_not(is_end))
    def _():
        last = jnp.where(is_lower, n - 1, 1)
        last_way = jnp.where(is_lower, 1, 0)
        skew = jnp.where(leads, (me - 1) * 2, 0)
        split = jnp.where(is_lower, n - 1, 1)
        share = PIECES // SLOT
        follows = jnp.logical_not(leads)

        def attend(i):
            attend_block(i)

        def multiply_three(c):
            multiply_piece(0, 3, cols(c))

        @pl.when(leads)
        def _():
            def both(c):
                @pl.when(c < PIECES)
                def _():
                    forward(1, me + 1, c)

                @pl.when(jnp.logical_and(c == PIECES // 2, me > 1))
                def _():
                    sent(1, me)
                    give_turn()

                @pl.when(c >= skew)
                def _():
                    forward(0, 0, c - skew)
                    multiply_three(c - skew)

            each(0, PIECES + skew, both)

        @pl.when(follows)
        def _():
            take_turn()
            way = jnp.where(is_lower, 0, 1)
            first = jnp.where(is_lower, 0, n - 1)
            second = jnp.where(is_lower, 2, 0)
            each(0, PIECES, lambda c: forward(way, first, c))

            @pl.when(me > 1)
            def _():
                pl.semaphore_wait(turn, 1)

            def then(c):
                forward(1 - way, second, c)
                multiply_three(c)

            each(0, PIECES, then)

        wait_tables()

        @pl.when(is_lower)
        def _():
            rest_of_own()

            def attend_forward(i):
                attend(i)
                each(i * share, (i + 1) * share, lambda c: forward(1, n - 1, c))

                @pl.when(jnp.logical_and(i == 1, leads))
                def _():
                    for block in range(2):
                        sent(0, block)
                        sent(1, block + 1)
                    give_turn()

            each(0, n - 1, attend_forward)

            def out_piece(c):
                project(0, 3, cols(c))

                @pl.when(c < PIECES - (n - 1) * share)
                def _():
                    forward(1, n - 1, c + (n - 1) * share)

            each(0, PIECES, out_piece)

        @pl.when(jnp.logical_not(is_lower))
        def _():
            attend(0)

            def out_piece(c):
                project(0, 1, cols(c))
                forward(0, 1, c)

            each(0, PIECES, out_piece)
            rest_of_own()

        def multiply_last(c):
            multiply_piece(3, 1, cols(c))

            @pl.when(functools.reduce(jnp.logical_and, (c == PIECES // 2, me > 1, leads)))
            def _():
                for block in range(2):
                    sent(0, block)
                give_turn()

        each(0, PIECES, multiply_last)
        each(split, n, attend)

        @pl.when(is_lower)
        def _():
            each(0, PIECES, lambda c: project(n - 1, 1, cols(c)))

            def stream(k):
                token = 2 + k // PIECES
                pass_on(token, lax.rem(k, PIECES))

                @pl.when(jnp.logical_and(k >= LAG, k < PIECES + LAG))
                def _():
                    pass_on(0, k - LAG)

            def stream_late(k):
                @pl.when(k < 2 * PIECES)
                def _():
                    pass_on(2 + k // PIECES, lax.rem(k, PIECES))

                @pl.when(k >= LATE)
                def _():
                    pass_on(0, k - LATE)

            @pl.when(leads)
            def _():
                each(0, PIECES + LATE, stream_late)

            @pl.when(follows)
            def _():
                each(0, 2 * PIECES, stream)

        @pl.when(jnp.logical_not(is_lower))
        def _():
            def out_piece(c):
                project(1, 3, cols(c))
                pass_on(0, c)

            each(0, PIECES, out_piece)

            def two(c):
                @pl.when(c < PIECES)
                def _():
                    pass_on(1, c)

                @pl.when(c >= LAG)
                def _():
                    pass_on(n - 1, c - LAG)

            each(0, PIECES + LAG, two)

        drain_gather(jnp.where(leads, 2, 0), jnp.where(leads, n - 1, 0))

        def finish(c):
            for way in range(2):
                sum_copy(way, me, c).wait_recv()
            out_ref[:, cols(c)] = (
                x_ref[:, cols(c)].astype(jnp.float32)
                + parts[me, :, cols(c)].astype(jnp.float32)
                + incoming[0, me, :, cols(c)].astype(jnp.float32)
                + incoming[1, me, :, cols(c)].astype(jnp.float32)
            ).astype(out_ref.dtype)

        each(0, PIECES, finish)

    def drain(token):
        @pl.when(token != me)
        def _():
            whole_copy(parts, rs_send.at[token], token).wait_send()

    each(0, n, drain)


def fused(layer_input, norm_gain, query_weight, key_weight, value_matrix, output_weight, keep_bits):
    n = lax.axis_size("tensor")
    rows, width = layer_input.shape
    length = n * rows
    half = HEAD_SIZE // 2
    freqs = theta_base ** (-(np.arange(half, dtype=np.float64) * 2.0) / HEAD_SIZE)
    angles = np.arange(length)[:, None] * freqs[None, :]
    cosine = np.concatenate([np.cos(angles), np.cos(angles)], axis=1).astype(np.float32)
    sine = np.concatenate([-np.sin(angles), np.sin(angles)], axis=1).astype(np.float32)
    heads = query_weight.shape[1] // HEAD_SIZE
    kv_heads = key_weight.shape[1] // HEAD_SIZE
    vmem = pl.BlockSpec(memory_space=pltpu.VMEM)
    hbm = pl.BlockSpec(memory_space=pltpu.HBM)
    bf16 = jnp.bfloat16
    weights = (query_weight, key_weight, value_matrix, output_weight)
    return pl.pallas_call(
        functools.partial(chain_kernel, n),
        out_shape=pltpu.VMEM((rows, width), bf16),
        in_specs=[hbm] * 9,
        out_specs=vmem,
        scratch_shapes=[
            pltpu.VMEM((rows, width), bf16),
            pltpu.VMEM((1, width), jnp.float32),
            pltpu.SMEM(keep_bits.shape[1:] + keep_bits.shape[:1], jnp.int32),
            pltpu.VMEM(cosine.shape, jnp.float32),
            pltpu.VMEM(sine.shape, jnp.float32),
        ]
        + [pltpu.VMEM(w.shape, bf16) for w in weights]
        + [
            pltpu.VMEM((n, rows, width), bf16),
            pltpu.VMEM((n, rows, width), bf16),
            pltpu.VMEM((2, n, rows, width), bf16),
            pltpu.VMEM((kv_heads, length, HEAD_SIZE), bf16),
            pltpu.VMEM((kv_heads, length, HEAD_SIZE), bf16),
            pltpu.VMEM((kv_heads, heads // kv_heads * rows, HEAD_SIZE), bf16),
            pltpu.VMEM((n, rows, heads * HEAD_SIZE), bf16),
            pltpu.VMEM((n, rows, (heads + 2 * kv_heads) * HEAD_SIZE), jnp.float32),
            pltpu.SemaphoreType.DMA((9,)),
            pltpu.SemaphoreType.DMA((2, n)),
            pltpu.SemaphoreType.DMA((n, PIECES)),
            pltpu.SemaphoreType.DMA((n,)),
            pltpu.SemaphoreType.DMA((2, n, PIECES)),
            pltpu.SemaphoreType.REGULAR,
        ],
        compiler_params=pltpu.CompilerParams(
            collective_id=0, has_side_effects=True, vmem_limit_bytes=60 * 2**20
        ),
    )(layer_input, norm_gain[None, :], keep_bits.transpose(1, 2, 0), cosine, sine, *weights)


def solution(mesh):
    in_specs = (
        P(("dp", "tensor"), None),
        P(),
        P(None, "tensor"),
        P(None, "tensor"),
        P(None, "tensor"),
        P("tensor", None),
        P(("dp", "tensor"), None, None),
    )
    out_specs = P(("dp", "tensor"), None)
    return jax.shard_map(
        on_device, mesh=mesh, in_specs=in_specs, out_specs=out_specs, check_vma=False
    )
```

```python
import functools

import jax
import jax.numpy as jnp
import numpy as np
from jax import lax
from jax.experimental import pallas as pl
from jax.experimental.pallas import tpu as pltpu
from jax.sharding import PartitionSpec as P

QUERY_HEADS = 32
KEY_VALUE_HEADS = 8
HEAD_SIZE = 128
BLOCK = 64


theta_base = 1000000.0


def as_sent(array):

    def short(part):
        return part.astype(jnp.bfloat16) if part.dtype == jnp.float32 else part

    return jax.tree.map(short, array)


def from_partner(array, axis, distance):
    return lax.ppermute(array, axis, [(i, i ^ 1 << distance) for i in range(lax.axis_size(axis))])


def apply_rotary(block, token_positions):
    half = block.shape[-1] // 2
    freqs = theta_base ** (-(jnp.arange(half, dtype=jnp.float32) * 2.0) / block.shape[-1])
    angles = token_positions[:, None] * freqs[None, :]
    cosine = jnp.cos(angles)
    sine = jnp.sin(angles)
    first = block[..., :half]
    second = block[..., half:]
    return jnp.concatenate(
        [first * cosine - second * sine, second * cosine + first * sine], axis=-1
    )


def join_pairs(mine, other, lowbit):
    ahead = jnp.concatenate([mine, other], axis=-1)
    behind = jnp.concatenate([other, mine], axis=-1)
    return jnp.where(lowbit, ahead, behind)


def attend(query, key_rows, value_rows, keep_bits):
    heads, sequence_length, width = query.shape
    count = min(8, max(1, sequence_length // 512))
    height = sequence_length // count
    divisor = jnp.sqrt(jnp.float32(HEAD_SIZE))
    results = []
    for number in range(count):
        first_row = number * height
        last_row = first_row + height
        scores = (
            jnp.einsum(
                "hqd,hkd->hqk",
                query[:, first_row:last_row],
                key_rows[:, :last_row],
                preferred_element_type=jnp.float32,
            )
            / divisor
        )
        causal = jnp.arange(last_row)[None, :] <= jnp.arange(first_row, last_row)[:, None]
        scores = jnp.where(causal[None], scores, jnp.float32(-1e30))
        highest = jnp.max(scores, axis=-1, keepdims=True)
        expo_terms = jnp.exp(scores - highest)
        weights = expo_terms / jnp.sum(expo_terms, axis=-1, keepdims=True)
        chosen_bits = keep_bits[
            :, first_row // BLOCK : last_row // BLOCK, : last_row // BLOCK
        ].astype(jnp.float32)
        keeper = jnp.broadcast_to(
            chosen_bits[:, :, None, :, None],
            (heads, height // BLOCK, BLOCK, last_row // BLOCK, BLOCK),
        ).reshape(heads, height, last_row)
        dropped = (weights * keeper / 0.9).astype(jnp.bfloat16)
        outcome = jnp.einsum(
            "hqk,hkd->hqd", dropped, value_rows[:, :last_row], preferred_element_type=jnp.float32
        )
        results.append(outcome.astype(jnp.bfloat16))
    return jnp.concatenate(results, axis=1)


def on_device(
    layer_input, norm_gain, query_weight, key_weight, value_matrix, output_weight, keep_bits
):
    devices = lax.axis_size("tensor")
    paired = lax.axis_size("dp") % 2 == 0
    if devices == CHAIN and paired and layer_input.shape[0] == BLOCK:
        return fused(
            layer_input,
            norm_gain,
            query_weight,
            key_weight,
            value_matrix,
            output_weight,
            keep_bits,
        )
    position = lax.axis_index("tensor")
    sharing = devices // KEY_VALUE_HEADS if devices > KEY_VALUE_HEADS else 1
    rounds = sharing.bit_length() - 1
    inputs = layer_input.astype(jnp.float32)
    scaled = lax.rsqrt(jnp.mean(inputs * inputs, axis=-1, keepdims=True) + 1e-05)
    normed = (inputs * scaled * norm_gain[None, :]).astype(jnp.bfloat16)
    query_cols = query_weight.shape[1]
    kv_cols = key_weight.shape[1]
    piece = lax.all_gather(normed, "tensor", axis=0, tiled=True)
    projected = jnp.concatenate(
        [
            jnp.dot(piece, query_weight, preferred_element_type=jnp.float32),
            jnp.dot(piece, key_weight, preferred_element_type=jnp.float32),
            jnp.dot(piece, value_matrix, preferred_element_type=jnp.float32),
        ],
        axis=1,
    )
    query_raw = projected[:, :query_cols]
    paired = jnp.stack(
        [projected[:, query_cols : query_cols + kv_cols], projected[:, query_cols + kv_cols :]]
    ).astype(jnp.bfloat16)
    for level in range(rounds):
        other = from_partner(as_sent(paired), "tensor", level).astype(paired.dtype)
        paired = join_pairs(paired, other, position >> level & 1 == 0)
    sequence_length = query_raw.shape[0]
    local_heads = query_cols // HEAD_SIZE
    local_kv = paired.shape[2] // HEAD_SIZE
    token_positions = jnp.arange(sequence_length).astype(jnp.float32)
    query = apply_rotary(
        query_raw.reshape(sequence_length, local_heads, HEAD_SIZE).transpose(1, 0, 2),
        token_positions,
    ).astype(jnp.bfloat16)
    key_rows = apply_rotary(
        paired[0]
        .astype(jnp.float32)
        .reshape(sequence_length, local_kv, HEAD_SIZE)
        .transpose(1, 0, 2),
        token_positions,
    ).astype(jnp.bfloat16)
    value_rows = paired[1].reshape(sequence_length, local_kv, HEAD_SIZE).transpose(1, 0, 2)
    query_group = QUERY_HEADS // KEY_VALUE_HEADS
    if local_heads >= query_group:
        key_rows = jnp.repeat(key_rows, query_group, axis=0)
        value_rows = jnp.repeat(value_rows, query_group, axis=0)
    else:
        key_rows = jnp.broadcast_to(key_rows, (local_heads, sequence_length, HEAD_SIZE))
        value_rows = jnp.broadcast_to(value_rows, (local_heads, sequence_length, HEAD_SIZE))
    heads = attend(query, key_rows, value_rows, keep_bits)
    heads_out = heads.transpose(1, 0, 2).reshape(sequence_length, query_cols)
    terms = jnp.dot(heads_out, output_weight, preferred_element_type=jnp.float32).astype(
        jnp.bfloat16
    )
    total = lax.psum_scatter(terms, "tensor", scatter_dimension=0, tiled=True).astype(jnp.float32)
    return (inputs + total).astype(jnp.bfloat16)


MESH = pl.DeviceIdType.MESH
CHAIN = 4
PIECES = 8
SLOT = 4
LAG = 4
TURN = 3


def chain_kernel(
    n,
    x_hbm,
    gain_hbm,
    keep_hbm,
    cos_hbm,
    sin_hbm,
    wq_hbm,
    wk_hbm,
    wv_hbm,
    wo_hbm,
    out_ref,
    x_ref,
    gain_ref,
    keep_ref,
    cos_ref,
    sin_ref,
    wq,
    wk,
    wv,
    wo,
    gathered,
    parts,
    incoming,
    keys,
    values,
    queries,
    joined,
    projected,
    load_sem,
    ag_send,
    ag_recv,
    rs_send,
    rs_recv,
    turn,
):
    me = lax.axis_index("tensor")
    rows, width = x_ref.shape
    length = n * rows
    step = width // PIECES
    heads = wq.shape[1] // HEAD_SIZE
    kv_heads = wk.shape[1] // HEAD_SIZE
    group = heads // kv_heads
    has_left = me > 0
    has_right = me < n - 1
    is_lower = me < n // 2
    is_end = jnp.logical_or(me == 0, me == n - 1)
    pair = lax.axis_index("dp")
    leads = lax.rem(pair, 2) == 1
    partner = jnp.where(leads, pair - 1, pair + 1)

    loads = [
        pltpu.make_async_copy(src, dst, load_sem.at[i])
        for i, (src, dst) in enumerate(
            (
                (x_hbm, x_ref),
                (gain_hbm, gain_ref),
                (keep_hbm, keep_ref),
                (wk_hbm, wk),
                (wv_hbm, wv),
                (wq_hbm, wq),
                (cos_hbm, cos_ref),
                (sin_hbm, sin_ref),
                (wo_hbm, wo),
            )
        )
    ]

    barrier = pltpu.get_barrier_semaphore()

    @pl.when(has_left)
    def _():
        pl.semaphore_signal(barrier, inc=1, device_id={"tensor": me - 1}, device_id_type=MESH)

    @pl.when(has_right)
    def _():
        pl.semaphore_signal(barrier, inc=1, device_id={"tensor": me + 1}, device_id_type=MESH)

    pl.semaphore_signal(barrier, inc=1, device_id={"dp": partner}, device_id_type=MESH)

    for load in loads[:3]:
        load.start()
    loads[0].wait()
    loads[1].wait()
    for load in loads[3:]:
        load.start()

    def slot(device, block):
        return lax.rem(block + jnp.where(device == 2, 2, 0), n)

    inputs = x_ref[...].astype(jnp.float32)
    scaled = lax.rsqrt(jnp.mean(inputs * inputs, axis=-1, keepdims=True) + 1e-05)
    gathered[slot(me, me)] = (inputs * scaled * gain_ref[...]).astype(jnp.bfloat16)

    pl.semaphore_wait(barrier, jnp.where(is_end, 2, 3))

    def cols(c):
        return pl.ds(pl.multiple_of(c * step, step), step)

    def pairs(k):
        return pl.ds(pl.multiple_of(k * 2 * step, 2 * step), 2 * step)

    def other(device, block):
        return jnp.where(block > device, block - 1, block)

    def gather_copy(way, block, c):
        to = me + 1 - 2 * way
        return pltpu.make_async_remote_copy(
            src_ref=gathered.at[slot(me, block), :, cols(c)],
            dst_ref=gathered.at[slot(to, block), :, cols(c)],
            send_sem=ag_send.at[block + way],
            recv_sem=ag_recv.at[other(to, block), c],
            device_id={"tensor": to},
            device_id_type=MESH,
        )

    def arrived(block, c):
        arrival(block, c)

    def arrival(block, c):
        piece = gathered.at[slot(me, block), :, cols(c)]
        pltpu.make_async_remote_copy(
            src_ref=piece,
            dst_ref=piece,
            send_sem=ag_send.at[0],
            recv_sem=ag_recv.at[other(me, block), c],
            device_id={"tensor": jnp.where(has_right, me + 1, me - 1)},
            device_id_type=MESH,
        ).wait_recv()

    def sum_copy(way, token, c):
        return pltpu.make_async_remote_copy(
            src_ref=parts.at[token, :, cols(c)],
            dst_ref=incoming.at[token + 1 - way, :, cols(c)],
            send_sem=rs_send.at[token],
            recv_sem=rs_recv.at[token + 1 - way, c],
            device_id={"tensor": me + 1 - 2 * way},
            device_id_type=MESH,
        )

    def whole_copy(buffer, sem, index):
        return pltpu.make_async_remote_copy(
            src_ref=buffer.at[index],
            dst_ref=buffer.at[index],
            send_sem=sem,
            recv_sem=ag_recv.at[0, 0],
            device_id={"tensor": jnp.where(has_right, me + 1, me - 1)},
            device_id_type=MESH,
        )

    def each(first, last, body):
        lax.fori_loop(first, last, lambda c, carry: (body(c), carry)[1], 0)

    early = jnp.where(me == 0, PIECES, jnp.where(leads, me * PIECES // 2, 0))

    def send_own():
        @pl.when(has_right)
        def _():
            each(0, early, lambda c: gather_copy(0, me, c).start())

        @pl.when(has_left)
        def _():
            each(0, PIECES, lambda c: gather_copy(1, me, c).start())

    pl.when(leads)(send_own)

    def take_turn():
        pl.semaphore_wait(turn, 1)

    def give_turn():
        pl.semaphore_signal(turn, inc=1, device_id={"dp": partner}, device_id_type=MESH)

    def rest_of_own():
        each(early, PIECES, lambda c: gather_copy(0, me, c).start())

    def forward(way, block, c):
        arrived(block, c)
        gather_copy(way, block, c).start()

    def rotated(t, cosine, sine):
        return t * cosine + pltpu.roll(t, HEAD_SIZE // 2, 1) * sine

    def multiply(first, count, where):
        block = gathered[pl.ds(first, count), :, where].reshape(count * rows, -1)
        spans = []
        at = 0
        for weight in (wq, wk, wv):
            product = jnp.dot(block, weight[where, :], preferred_element_type=jnp.float32)
            spans.append((slice(at, at + weight.shape[1]), product.reshape(count, rows, -1)))
            at += weight.shape[1]
        return spans

    def multiply_whole(first, between):
        block = gathered[first]
        at = 0
        for weight in (wq, wk, wv):
            span = slice(at, at + weight.shape[1])
            projected[first, :, span] = jnp.dot(
                block, weight[...], preferred_element_type=jnp.float32
            )
            if at == 0:
                between()
            at += weight.shape[1]

    def multiply_piece(first, count, where):
        for span, product in multiply(first, count, where):
            projected[pl.ds(first, count), :, span] += product

    def attend_block(token, length=length):
        here = slot(me, token)
        first_row = pl.multiple_of(token * rows, rows)
        where = pl.ds(first_row, rows)
        q_cols, kv_cols = wq.shape[1], wk.shape[1]
        cosine = cos_ref[where, :]
        sine = sin_ref[where, :]
        key_raw = (
            projected[here, :, q_cols : q_cols + kv_cols].astype(jnp.bfloat16).astype(jnp.float32)
        )
        value = projected[here, :, q_cols + kv_cols :].astype(jnp.bfloat16)
        for g in range(kv_heads):
            span = slice(g * HEAD_SIZE, (g + 1) * HEAD_SIZE)
            keys[g, where, :] = rotated(key_raw[:, span], cosine, sine).astype(jnp.bfloat16)
            values[g, where, :] = value[:, span]
        for g in range(kv_heads):
            wide = slice(g * group * HEAD_SIZE, (g + 1) * group * HEAD_SIZE)
            raw = projected[here, :, wide]
            for h in range(group):
                one = raw[:, h * HEAD_SIZE : (h + 1) * HEAD_SIZE]
                queries[g, h * rows : (h + 1) * rows, :] = rotated(one, cosine, sine).astype(
                    jnp.bfloat16
                )
        column = lax.broadcasted_iota(jnp.int32, (rows, length), 1)
        row = lax.broadcasted_iota(jnp.int32, (rows, length), 0) + first_row
        causal = column <= row
        which = lax.broadcasted_iota(jnp.int32, (1, length), 1) // BLOCK
        for g in range(kv_heads):
            scores = lax.dot_general(
                queries[g], keys[g, :length], (((1,), (1,)), ((), ())), preferred_element_type=jnp.float32
            ) * np.float32(1.0 / np.sqrt(HEAD_SIZE))
            dropped = []
            for h in range(group):
                one = jnp.where(causal, scores[h * rows : (h + 1) * rows], jnp.float32(-1e30))
                highest = jnp.max(one, axis=-1, keepdims=True)
                terms = jnp.exp(one - highest)
                inverse = 1.0 / (jnp.sum(terms, axis=-1, keepdims=True) * jnp.float32(0.9))
                keeper = jnp.zeros((1, length), jnp.float32)
                for j in range(length // BLOCK):
                    bit = keep_ref[token, j, g * group + h].astype(jnp.float32)
                    keeper = jnp.where(which == j, bit, keeper)
                dropped.append((terms * inverse * keeper).astype(jnp.bfloat16))
            result = jnp.dot(
                jnp.concatenate(dropped, axis=0), values[g, :length], preferred_element_type=jnp.float32
            ).astype(jnp.bfloat16)
            for h in range(group):
                at = (g * group + h) * HEAD_SIZE
                joined[token, :, at : at + HEAD_SIZE] = result[h * rows : (h + 1) * rows]

    def project(first, count, where):
        mixed = joined[pl.ds(first, count)].reshape(count * rows, -1)
        parts[pl.ds(first, count), :, where] = (
            jnp.dot(mixed, wo[:, where], preferred_element_type=jnp.float32)
            .astype(jnp.bfloat16)
            .reshape(count, rows, -1)
        )

    def pass_on(token, c):
        way = jnp.where(me < token, 0, 1)
        sum_copy(way, token, c).wait_recv()
        total = parts[token, :, cols(c)].astype(jnp.float32) + incoming[
            token + 1 - way, :, cols(c)
        ].astype(jnp.float32)
        parts[token, :, cols(c)] = total.astype(jnp.bfloat16)
        sum_copy(way, token, c).start()

    keys[...] = jnp.zeros_like(keys)
    values[...] = jnp.zeros_like(values)
    projected[...] = jnp.zeros_like(projected)
    def wait_inputs():
        for load in loads[3:6]:
            load.wait()


    def wait_tables():
        for load in loads[6:] + loads[2:3]:
            load.wait()

    def drain_gather():
        def drain(block):
            @pl.when(jnp.logical_and(block <= me, has_right))
            def _():
                sent(0, block)

            @pl.when(jnp.logical_and(block >= me, has_left))
            def _():
                sent(1, block)

        each(0, n, drain)

    def sent(way, block):
        whole_copy(gathered, ag_send.at[block + way], block).wait_send()

    @pl.when(is_end)
    def _():
        way = jnp.where(me == 0, 0, 1)
        wait_inputs()

        @pl.when(jnp.logical_not(leads))
        def _():
            take_turn()
            send_own()

        multiply_whole(me, lambda: pl.when(leads)(give_turn))
        wait_tables()

        ahead = jnp.where(jnp.logical_and(leads, me > 0), n - 2, -1)

        def stream(i):
            def piece(k):
                arrived(i, 2 * k)
                arrived(i, 2 * k + 1)
                multiply_piece(i, 1, pairs(k))

            each(0, PIECES // 2, piece)

        @pl.when(ahead >= 0)
        def _():
            stream(ahead)

        def iteration(i, carry):
            @pl.when(jnp.logical_and(i != me, i != ahead))
            def _():
                stream(i)

            @pl.when(i == 0)
            def _():
                attend_block(0, rows)

            @pl.when(i > 0)
            def _():
                attend_block(i)

            def out_piece(k):
                project(i, 1, pairs(k))
                sum_copy(way, i, 2 * k).start()
                sum_copy(way, i, 2 * k + 1).start()

            @pl.when(i != me)
            def _():
                each(0, PIECES // 2, out_piece)

            return carry

        lax.fori_loop(0, n, iteration, 0)

        def out_own(k):
            project(me, 1, pairs(k))

        each(0, PIECES // 2, out_own)
        drain_gather()

        def finish(c):
            sum_copy(1 - way, me, c).wait_recv()
            out_ref[:, cols(c)] = (
                x_ref[:, cols(c)].astype(jnp.float32)
                + parts[me, :, cols(c)].astype(jnp.float32)
                + incoming[me + way, :, cols(c)].astype(jnp.float32)
            ).astype(out_ref.dtype)

        each(0, PIECES, finish)

    @pl.when(jnp.logical_not(is_end))
    def _():
        last = jnp.where(is_lower, n - 1, 1)
        last_way = jnp.where(is_lower, 1, 0)
        up_lag = jnp.where(is_lower, 0, 3)
        down_lag = jnp.where(is_lower, 2, 0)
        lag = up_lag + down_lag
        split = jnp.where(is_lower, n - 1, 1)
        share = PIECES // SLOT
        follows = jnp.logical_not(leads)

        def attend(i):
            attend_block(i)

        def multiply_three(c):
            multiply_piece(0, 3, cols(c))

        @pl.when(leads)
        def _():
            def both(c):
                @pl.when(jnp.logical_and(c >= up_lag, c < PIECES + up_lag))
                def _():
                    forward(0, 0, c - up_lag)

                @pl.when(jnp.logical_and(c >= down_lag, c < PIECES + down_lag))
                def _():
                    forward(1, me + 1, c - down_lag)

                @pl.when(jnp.logical_and(c == PIECES, is_lower))
                def _():
                    rest_of_own()

                @pl.when(c == lag)
                def _():
                    wait_inputs()

                @pl.when(c >= lag)
                def _():
                    multiply_three(c - lag)

            each(0, PIECES + lag, both)

            pl.when(me > 1)(give_turn)


        @pl.when(follows)
        def _():
            wait_inputs()
            way = jnp.where(is_lower, 0, 1)
            first = jnp.where(is_lower, 0, n - 1)
            second = jnp.where(is_lower, 2, 0)
            take_turn()
            pl.when(me > 1)(send_own)
            each(0, PIECES, lambda c: forward(way, first, c))
            pl.when(is_lower)(rest_of_own)
            take_turn()
            pl.when(is_lower)(send_own)

            def then(c):
                forward(1 - way, second, c)
                multiply_three(c)

            each(0, PIECES, then)

        wait_tables()

        @pl.when(is_lower)
        def _():
            def attend_forward(i):
                attend(i)
                each(i * share, (i + 1) * share, lambda c: forward(1, n - 1, c))
                pl.when(jnp.logical_and(i == 0, leads))(give_turn)

            each(0, n - 1, attend_forward)
            pl.when(follows)(give_turn)


            def out_piece(c):
                project(0, 3, cols(c))

                @pl.when(c < PIECES - (n - 1) * share)
                def _():
                    forward(1, n - 1, c + (n - 1) * share)

                pl.when(jnp.logical_and(c == TURN, leads))(give_turn)

            each(0, PIECES, out_piece)


        @pl.when(jnp.logical_not(is_lower))
        def _():
            each(0, PIECES // 2, lambda c: forward(0, 1, c))
            attend(0)

            def out_piece(c):
                @pl.when(c < PIECES // 2)
                def _():
                    forward(0, 1, c + PIECES // 2)

                project(0, 1, cols(c))

            each(0, PIECES, out_piece)
            rest_of_own()
            pl.when(leads)(give_turn)

        def multiply_last(c):
            multiply_piece(3, 1, cols(c))

        each(0, PIECES, multiply_last)
        each(split, n, attend)


        @pl.when(is_lower)
        def _():
            each(0, PIECES, lambda c: project(n - 1, 1, cols(c)))

            def stream(k):
                token = 2 + k // PIECES
                pass_on(token, lax.rem(k, PIECES))

                @pl.when(jnp.logical_and(k >= LAG, k < PIECES + LAG))
                def _():
                    pass_on(0, k - LAG)

            @pl.when(leads)
            def _():
                take_turn()
                each(0, PIECES, lambda c: pass_on(2, c))
                each(0, PIECES, lambda c: pass_on(n - 1, c))
                take_turn()
                each(0, PIECES, lambda c: pass_on(0, c))

            @pl.when(follows)
            def _():
                give_turn()
                each(0, 2 * PIECES, stream)

        @pl.when(jnp.logical_not(is_lower))
        def _():
            def out_piece(c):
                project(1, 3, cols(c))
                pass_on(0, c)
                pl.when(jnp.logical_and(c == 1, follows))(give_turn)

            each(0, PIECES, out_piece)

            def two(c):
                @pl.when(c < PIECES)
                def _():
                    pass_on(1, c)

                @pl.when(c >= LAG)
                def _():
                    pass_on(n - 1, c - LAG)

            @pl.when(leads)
            def _():
                each(0, PIECES, lambda c: pass_on(1, c))
                take_turn()
                each(0, PIECES, lambda c: pass_on(n - 1, c))

            @pl.when(follows)
            def _():
                each(0, PIECES + LAG, two)

        drain_gather()

        def finish(c):
            for way in range(2):
                sum_copy(way, me, c).wait_recv()
            out_ref[:, cols(c)] = (
                x_ref[:, cols(c)].astype(jnp.float32)
                + parts[me, :, cols(c)].astype(jnp.float32)
                + incoming[me + 1, :, cols(c)].astype(jnp.float32)
                + incoming[me, :, cols(c)].astype(jnp.float32)
            ).astype(out_ref.dtype)

        each(0, PIECES, finish)

    def drain(token):
        @pl.when(token != me)
        def _():
            whole_copy(parts, rs_send.at[token], token).wait_send()

    each(0, n, drain)


def fused(layer_input, norm_gain, query_weight, key_weight, value_matrix, output_weight, keep_bits):
    n = lax.axis_size("tensor")
    rows, width = layer_input.shape
    length = n * rows
    half = HEAD_SIZE // 2
    freqs = theta_base ** (-(np.arange(half, dtype=np.float64) * 2.0) / HEAD_SIZE)
    angles = np.arange(length)[:, None] * freqs[None, :]
    cosine = np.concatenate([np.cos(angles), np.cos(angles)], axis=1).astype(np.float32)
    sine = np.concatenate([-np.sin(angles), np.sin(angles)], axis=1).astype(np.float32)
    heads = query_weight.shape[1] // HEAD_SIZE
    kv_heads = key_weight.shape[1] // HEAD_SIZE
    vmem = pl.BlockSpec(memory_space=pltpu.VMEM)
    hbm = pl.BlockSpec(memory_space=pltpu.HBM)
    bf16 = jnp.bfloat16
    weights = (query_weight, key_weight, value_matrix, output_weight)
    return pl.pallas_call(
        functools.partial(chain_kernel, n),
        out_shape=pltpu.VMEM((rows, width), bf16),
        in_specs=[hbm] * 9,
        out_specs=vmem,
        scratch_shapes=[
            pltpu.VMEM((rows, width), bf16),
            pltpu.VMEM((1, width), jnp.float32),
            pltpu.SMEM(keep_bits.shape[1:] + keep_bits.shape[:1], jnp.int32),
            pltpu.VMEM(cosine.shape, jnp.float32),
            pltpu.VMEM(sine.shape, jnp.float32),
        ]
        + [pltpu.VMEM(w.shape, bf16) for w in weights]
        + [
            pltpu.VMEM((n, rows, width), bf16),
            pltpu.VMEM((n, rows, width), bf16),
            pltpu.VMEM((n + 1, rows, width), bf16),
            pltpu.VMEM((kv_heads, length, HEAD_SIZE), bf16),
            pltpu.VMEM((kv_heads, length, HEAD_SIZE), bf16),
            pltpu.VMEM((kv_heads, heads // kv_heads * rows, HEAD_SIZE), bf16),
            pltpu.VMEM((n, rows, heads * HEAD_SIZE), bf16),
            pltpu.VMEM((n, rows, (heads + 2 * kv_heads) * HEAD_SIZE), jnp.float32),
            pltpu.SemaphoreType.DMA((9,)),
            pltpu.SemaphoreType.DMA((n + 1,)),
            pltpu.SemaphoreType.DMA((n - 1, PIECES)),
            pltpu.SemaphoreType.DMA((n,)),
            pltpu.SemaphoreType.DMA((n + 1, PIECES)),
            pltpu.SemaphoreType.REGULAR,
        ],
        compiler_params=pltpu.CompilerParams(
            collective_id=0, has_side_effects=True, vmem_limit_bytes=60 * 2**20
        ),
    )(layer_input, norm_gain[None, :], keep_bits.transpose(1, 2, 0), cosine, sine, *weights)


def solution(mesh):
    in_specs = (
        P(("dp", "tensor"), None),
        P(),
        P(None, "tensor"),
        P(None, "tensor"),
        P(None, "tensor"),
        P("tensor", None),
        P(("dp", "tensor"), None, None),
    )
    out_specs = P(("dp", "tensor"), None)
    return jax.shard_map(
        on_device, mesh=mesh, in_specs=in_specs, out_specs=out_specs, check_vma=False
    )
```

```python
import functools

import jax
import jax.numpy as jnp
import numpy as np
from jax import lax
from jax.experimental import pallas as pl
from jax.experimental.pallas import tpu as pltpu
from jax.sharding import PartitionSpec as P

QUERY_HEADS = 32
KEY_VALUE_HEADS = 8
HEAD_SIZE = 128
BLOCK = 64


theta_base = 1000000.0


def as_sent(array):

    def short(part):
        return part.astype(jnp.bfloat16) if part.dtype == jnp.float32 else part

    return jax.tree.map(short, array)


def from_partner(array, axis, distance):
    return lax.ppermute(array, axis, [(i, i ^ 1 << distance) for i in range(lax.axis_size(axis))])


def apply_rotary(block, token_positions):
    half = block.shape[-1] // 2
    freqs = theta_base ** (-(jnp.arange(half, dtype=jnp.float32) * 2.0) / block.shape[-1])
    angles = token_positions[:, None] * freqs[None, :]
    cosine = jnp.cos(angles)
    sine = jnp.sin(angles)
    first = block[..., :half]
    second = block[..., half:]
    return jnp.concatenate(
        [first * cosine - second * sine, second * cosine + first * sine], axis=-1
    )


def join_pairs(mine, other, lowbit):
    ahead = jnp.concatenate([mine, other], axis=-1)
    behind = jnp.concatenate([other, mine], axis=-1)
    return jnp.where(lowbit, ahead, behind)


def attend(query, key_rows, value_rows, keep_bits):
    heads, sequence_length, width = query.shape
    count = min(8, max(1, sequence_length // 512))
    height = sequence_length // count
    divisor = jnp.sqrt(jnp.float32(HEAD_SIZE))
    results = []
    for number in range(count):
        first_row = number * height
        last_row = first_row + height
        scores = (
            jnp.einsum(
                "hqd,hkd->hqk",
                query[:, first_row:last_row],
                key_rows[:, :last_row],
                preferred_element_type=jnp.float32,
            )
            / divisor
        )
        causal = jnp.arange(last_row)[None, :] <= jnp.arange(first_row, last_row)[:, None]
        scores = jnp.where(causal[None], scores, jnp.float32(-1e30))
        highest = jnp.max(scores, axis=-1, keepdims=True)
        expo_terms = jnp.exp(scores - highest)
        weights = expo_terms / jnp.sum(expo_terms, axis=-1, keepdims=True)
        chosen_bits = keep_bits[
            :, first_row // BLOCK : last_row // BLOCK, : last_row // BLOCK
        ].astype(jnp.float32)
        keeper = jnp.broadcast_to(
            chosen_bits[:, :, None, :, None],
            (heads, height // BLOCK, BLOCK, last_row // BLOCK, BLOCK),
        ).reshape(heads, height, last_row)
        dropped = (weights * keeper / 0.9).astype(jnp.bfloat16)
        outcome = jnp.einsum(
            "hqk,hkd->hqd", dropped, value_rows[:, :last_row], preferred_element_type=jnp.float32
        )
        results.append(outcome.astype(jnp.bfloat16))
    return jnp.concatenate(results, axis=1)


def on_device(
    layer_input, norm_gain, query_weight, key_weight, value_matrix, output_weight, keep_bits
):
    devices = lax.axis_size("tensor")
    paired = lax.axis_size("dp") % 2 == 0
    if devices == CHAIN and paired and layer_input.shape[0] == BLOCK:
        return fused(
            layer_input,
            norm_gain,
            query_weight,
            key_weight,
            value_matrix,
            output_weight,
            keep_bits,
        )
    position = lax.axis_index("tensor")
    sharing = devices // KEY_VALUE_HEADS if devices > KEY_VALUE_HEADS else 1
    rounds = sharing.bit_length() - 1
    inputs = layer_input.astype(jnp.float32)
    scaled = lax.rsqrt(jnp.mean(inputs * inputs, axis=-1, keepdims=True) + 1e-05)
    normed = (inputs * scaled * norm_gain[None, :]).astype(jnp.bfloat16)
    query_cols = query_weight.shape[1]
    kv_cols = key_weight.shape[1]
    piece = lax.all_gather(normed, "tensor", axis=0, tiled=True)
    projected = jnp.concatenate(
        [
            jnp.dot(piece, query_weight, preferred_element_type=jnp.float32),
            jnp.dot(piece, key_weight, preferred_element_type=jnp.float32),
            jnp.dot(piece, value_matrix, preferred_element_type=jnp.float32),
        ],
        axis=1,
    )
    query_raw = projected[:, :query_cols]
    paired = jnp.stack(
        [projected[:, query_cols : query_cols + kv_cols], projected[:, query_cols + kv_cols :]]
    ).astype(jnp.bfloat16)
    for level in range(rounds):
        other = from_partner(as_sent(paired), "tensor", level).astype(paired.dtype)
        paired = join_pairs(paired, other, position >> level & 1 == 0)
    sequence_length = query_raw.shape[0]
    local_heads = query_cols // HEAD_SIZE
    local_kv = paired.shape[2] // HEAD_SIZE
    token_positions = jnp.arange(sequence_length).astype(jnp.float32)
    query = apply_rotary(
        query_raw.reshape(sequence_length, local_heads, HEAD_SIZE).transpose(1, 0, 2),
        token_positions,
    ).astype(jnp.bfloat16)
    key_rows = apply_rotary(
        paired[0]
        .astype(jnp.float32)
        .reshape(sequence_length, local_kv, HEAD_SIZE)
        .transpose(1, 0, 2),
        token_positions,
    ).astype(jnp.bfloat16)
    value_rows = paired[1].reshape(sequence_length, local_kv, HEAD_SIZE).transpose(1, 0, 2)
    query_group = QUERY_HEADS // KEY_VALUE_HEADS
    if local_heads >= query_group:
        key_rows = jnp.repeat(key_rows, query_group, axis=0)
        value_rows = jnp.repeat(value_rows, query_group, axis=0)
    else:
        key_rows = jnp.broadcast_to(key_rows, (local_heads, sequence_length, HEAD_SIZE))
        value_rows = jnp.broadcast_to(value_rows, (local_heads, sequence_length, HEAD_SIZE))
    heads = attend(query, key_rows, value_rows, keep_bits)
    heads_out = heads.transpose(1, 0, 2).reshape(sequence_length, query_cols)
    terms = jnp.dot(heads_out, output_weight, preferred_element_type=jnp.float32).astype(
        jnp.bfloat16
    )
    total = lax.psum_scatter(terms, "tensor", scatter_dimension=0, tiled=True).astype(jnp.float32)
    return (inputs + total).astype(jnp.bfloat16)


MESH = pl.DeviceIdType.MESH
CHAIN = 4
PIECES = 8
SLOT = 4
HALVES = 2
LAG = 4
TURN = 3


def chain_kernel(
    n,
    x_hbm,
    gain_hbm,
    keep_hbm,
    cos_hbm,
    sin_hbm,
    wq_hbm,
    wk_hbm,
    wv_hbm,
    wo_hbm,
    out_ref,
    x_ref,
    gain_ref,
    keep_ref,
    cos_ref,
    sin_ref,
    wq,
    wk,
    wv,
    wo,
    gathered,
    parts,
    incoming,
    keys,
    values,
    queries,
    joined,
    projected,
    load_sem,
    ag_send,
    ag_recv,
    rs_send,
    rs_recv,
    turn,
):
    me = lax.axis_index("tensor")
    rows, width = x_ref.shape
    length = n * rows
    step = width // PIECES
    heads = wq.shape[1] // HEAD_SIZE
    kv_heads = wk.shape[1] // HEAD_SIZE
    group = heads // kv_heads
    has_left = me > 0
    has_right = me < n - 1
    is_lower = me < n // 2
    is_end = jnp.logical_or(me == 0, me == n - 1)
    pair = lax.axis_index("dp")
    leads = lax.rem(pair, 2) == 1
    partner = jnp.where(leads, pair - 1, pair + 1)

    loads = [
        pltpu.make_async_copy(src, dst, load_sem.at[i])
        for i, (src, dst) in enumerate(
            (
                (x_hbm, x_ref),
                (gain_hbm, gain_ref),
                (keep_hbm, keep_ref),
                (wk_hbm, wk),
                (wv_hbm, wv),
                (wq_hbm, wq),
                (cos_hbm, cos_ref),
                (sin_hbm, sin_ref),
                (wo_hbm, wo),
            )
        )
    ]

    barrier = pltpu.get_barrier_semaphore()

    @pl.when(has_left)
    def _():
        pl.semaphore_signal(barrier, inc=1, device_id={"tensor": me - 1}, device_id_type=MESH)

    @pl.when(has_right)
    def _():
        pl.semaphore_signal(barrier, inc=1, device_id={"tensor": me + 1}, device_id_type=MESH)

    pl.semaphore_signal(barrier, inc=1, device_id={"dp": partner}, device_id_type=MESH)

    for load in loads[:3]:
        load.start()
    loads[0].wait()
    loads[1].wait()
    for load in loads[3:]:
        load.start()

    def slot(device, block):
        return lax.rem(block + jnp.where(device == 2, 2, 0), n)

    inputs = x_ref[...].astype(jnp.float32)
    scaled = lax.rsqrt(jnp.mean(inputs * inputs, axis=-1, keepdims=True) + 1e-05)
    gathered[slot(me, me)] = (inputs * scaled * gain_ref[...]).astype(jnp.bfloat16)

    pl.semaphore_wait(barrier, jnp.where(is_end, 2, 3))

    def cols(c):
        return pl.ds(pl.multiple_of(c * step, step), step)

    def pairs(k):
        return pl.ds(pl.multiple_of(k * 2 * step, 2 * step), 2 * step)

    def other(device, block):
        return jnp.where(block > device, block - 1, block)

    def gather_copy(way, block, c):
        to = me + 1 - 2 * way
        return pltpu.make_async_remote_copy(
            src_ref=gathered.at[slot(me, block), :, cols(c)],
            dst_ref=gathered.at[slot(to, block), :, cols(c)],
            send_sem=ag_send.at[block + way],
            recv_sem=ag_recv.at[other(to, block), c],
            device_id={"tensor": to},
            device_id_type=MESH,
        )

    def arrived(block, c):
        arrival(block, c)

    def arrival(block, c):
        piece = gathered.at[slot(me, block), :, cols(c)]
        pltpu.make_async_remote_copy(
            src_ref=piece,
            dst_ref=piece,
            send_sem=ag_send.at[0],
            recv_sem=ag_recv.at[other(me, block), c],
            device_id={"tensor": jnp.where(has_right, me + 1, me - 1)},
            device_id_type=MESH,
        ).wait_recv()

    def sum_copy(way, token, c):
        return pltpu.make_async_remote_copy(
            src_ref=parts.at[token, :, cols(c)],
            dst_ref=incoming.at[token + 1 - way, :, cols(c)],
            send_sem=rs_send.at[token],
            recv_sem=rs_recv.at[token + 1 - way, c],
            device_id={"tensor": me + 1 - 2 * way},
            device_id_type=MESH,
        )

    def half_cols(c, h):
        size = step // HALVES
        return pl.ds(pl.multiple_of(c * step + h * size, size), size)

    def half_copy(c, h):
        return pltpu.make_async_remote_copy(
            src_ref=parts.at[n - 1, :, half_cols(c, h)],
            dst_ref=incoming.at[n, :, half_cols(c, h)],
            send_sem=rs_send.at[n - 1],
            recv_sem=rs_recv.at[n + h, c],
            device_id={"tensor": jnp.where(has_right, me + 1, me - 1)},
            device_id_type=MESH,
        )

    def whole_copy(buffer, sem, index):
        return pltpu.make_async_remote_copy(
            src_ref=buffer.at[index],
            dst_ref=buffer.at[index],
            send_sem=sem,
            recv_sem=ag_recv.at[0, 0],
            device_id={"tensor": jnp.where(has_right, me + 1, me - 1)},
            device_id_type=MESH,
        )

    def each(first, last, body):
        lax.fori_loop(first, last, lambda c, carry: (body(c), carry)[1], 0)

    early = jnp.where(me == 0, PIECES, jnp.where(leads, me * PIECES // 4, 0))

    def send_own():
        @pl.when(has_right)
        def _():
            each(0, early, lambda c: gather_copy(0, me, c).start())

        @pl.when(has_left)
        def _():
            each(0, PIECES, lambda c: gather_copy(1, me, c).start())

    pl.when(leads)(send_own)

    def take_turn():
        pl.semaphore_wait(turn, 1)

    def give_turn():
        pl.semaphore_signal(turn, inc=1, device_id={"dp": partner}, device_id_type=MESH)

    def rest_of_own():
        each(early, PIECES, lambda c: gather_copy(0, me, c).start())

    def forward(way, block, c):
        arrived(block, c)
        gather_copy(way, block, c).start()

    def rotated(t, cosine, sine):
        return t * cosine + pltpu.roll(t, HEAD_SIZE // 2, 1) * sine

    def multiply(first, count, where):
        block = gathered[pl.ds(first, count), :, where].reshape(count * rows, -1)
        spans = []
        at = 0
        for weight in (wq, wk, wv):
            product = jnp.dot(block, weight[where, :], preferred_element_type=jnp.float32)
            spans.append((slice(at, at + weight.shape[1]), product.reshape(count, rows, -1)))
            at += weight.shape[1]
        return spans

    def multiply_whole(first, between):
        block = gathered[first]
        at = 0
        for weight in (wq, wk, wv):
            span = slice(at, at + weight.shape[1])
            projected[first, :, span] = jnp.dot(
                block, weight[...], preferred_element_type=jnp.float32
            )
            if at == 0:
                between()
            at += weight.shape[1]

    def multiply_piece(first, count, where):
        for span, product in multiply(first, count, where):
            projected[pl.ds(first, count), :, span] += product

    def attend_block(token, length=length):
        here = slot(me, token)
        first_row = pl.multiple_of(token * rows, rows)
        where = pl.ds(first_row, rows)
        q_cols, kv_cols = wq.shape[1], wk.shape[1]
        cosine = cos_ref[where, :]
        sine = sin_ref[where, :]
        key_raw = (
            projected[here, :, q_cols : q_cols + kv_cols].astype(jnp.bfloat16).astype(jnp.float32)
        )
        value = projected[here, :, q_cols + kv_cols :].astype(jnp.bfloat16)
        for g in range(kv_heads):
            span = slice(g * HEAD_SIZE, (g + 1) * HEAD_SIZE)
            keys[g, where, :] = rotated(key_raw[:, span], cosine, sine).astype(jnp.bfloat16)
            values[g, where, :] = value[:, span]
        for g in range(kv_heads):
            wide = slice(g * group * HEAD_SIZE, (g + 1) * group * HEAD_SIZE)
            raw = projected[here, :, wide]
            for h in range(group):
                one = raw[:, h * HEAD_SIZE : (h + 1) * HEAD_SIZE]
                queries[g, h * rows : (h + 1) * rows, :] = rotated(one, cosine, sine).astype(
                    jnp.bfloat16
                )
        column = lax.broadcasted_iota(jnp.int32, (rows, length), 1)
        row = lax.broadcasted_iota(jnp.int32, (rows, length), 0) + first_row
        causal = column <= row
        which = lax.broadcasted_iota(jnp.int32, (1, length), 1) // BLOCK
        for g in range(kv_heads):
            scores = lax.dot_general(
                queries[g], keys[g, :length], (((1,), (1,)), ((), ())), preferred_element_type=jnp.float32
            ) * np.float32(1.0 / np.sqrt(HEAD_SIZE))
            dropped = []
            for h in range(group):
                one = jnp.where(causal, scores[h * rows : (h + 1) * rows], jnp.float32(-1e30))
                highest = jnp.max(one, axis=-1, keepdims=True)
                terms = jnp.exp(one - highest)
                inverse = 1.0 / (jnp.sum(terms, axis=-1, keepdims=True) * jnp.float32(0.9))
                keeper = jnp.zeros((1, length), jnp.float32)
                for j in range(length // BLOCK):
                    bit = keep_ref[token, j, g * group + h].astype(jnp.float32)
                    keeper = jnp.where(which == j, bit, keeper)
                dropped.append((terms * inverse * keeper).astype(jnp.bfloat16))
            result = jnp.dot(
                jnp.concatenate(dropped, axis=0), values[g, :length], preferred_element_type=jnp.float32
            ).astype(jnp.bfloat16)
            for h in range(group):
                at = (g * group + h) * HEAD_SIZE
                joined[token, :, at : at + HEAD_SIZE] = result[h * rows : (h + 1) * rows]

    def project(first, count, where):
        mixed = joined[pl.ds(first, count)].reshape(count * rows, -1)
        parts[pl.ds(first, count), :, where] = (
            jnp.dot(mixed, wo[:, where], preferred_element_type=jnp.float32)
            .astype(jnp.bfloat16)
            .reshape(count, rows, -1)
        )

    def pass_on(token, c):
        way = jnp.where(me < token, 0, 1)
        sum_copy(way, token, c).wait_recv()
        total = parts[token, :, cols(c)].astype(jnp.float32) + incoming[
            token + 1 - way, :, cols(c)
        ].astype(jnp.float32)
        parts[token, :, cols(c)] = total.astype(jnp.bfloat16)
        sum_copy(way, token, c).start()

    keys[...] = jnp.zeros_like(keys)
    values[...] = jnp.zeros_like(values)
    projected[...] = jnp.zeros_like(projected)
    def pass_last(c):
        for h in range(HALVES):
            where = half_cols(c, h)
            half_copy(c, h).wait_recv()
            total = parts[n - 1, :, where].astype(jnp.float32) + incoming[n, :, where].astype(
                jnp.float32
            )
            parts[n - 1, :, where] = total.astype(jnp.bfloat16)
            half_copy(c, h).start()

    def wait_inputs():
        for load in loads[3:6]:
            load.wait()


    def wait_tables():
        for load in loads[6:] + loads[2:3]:
            load.wait()

    def drain_gather():
        def drain(block):
            @pl.when(jnp.logical_and(block <= me, has_right))
            def _():
                sent(0, block)

            @pl.when(jnp.logical_and(block >= me, has_left))
            def _():
                sent(1, block)

        each(0, n, drain)

    def sent(way, block):
        whole_copy(gathered, ag_send.at[block + way], block).wait_send()

    @pl.when(is_end)
    def _():
        way = jnp.where(me == 0, 0, 1)
        wait_inputs()

        @pl.when(jnp.logical_not(leads))
        def _():
            take_turn()
            send_own()

        multiply_whole(me, lambda: pl.when(leads)(give_turn))
        wait_tables()


        def stream(i):
            def piece(k):
                arrived(i, 2 * k)
                arrived(i, 2 * k + 1)
                multiply_piece(i, 1, pairs(k))

            each(0, PIECES // 2, piece)

        def iteration(i, carry):
            @pl.when(i != me)
            def _():
                stream(i)

            @pl.when(i == 0)
            def _():
                attend_block(0, rows)

            @pl.when(i > 0)
            def _():
                attend_block(i)

            def out_piece(k):
                project(i, 1, pairs(k))
                longest = jnp.logical_and(me == 0, i == n - 1)

                @pl.when(longest)
                def _():
                    for c in (2 * k, 2 * k + 1):
                        for h in range(HALVES):
                            half_copy(c, h).start()

                @pl.when(jnp.logical_not(longest))
                def _():
                    for c in (2 * k, 2 * k + 1):
                        sum_copy(way, i, c).start()

            @pl.when(i != me)
            def _():
                each(0, PIECES // 2, out_piece)

            return carry

        lax.fori_loop(0, n, iteration, 0)

        def out_own(k):
            project(me, 1, pairs(k))

        each(0, PIECES // 2, out_own)
        drain_gather()

        def finish(c):
            @pl.when(me > 0)
            def _():
                for h in range(HALVES):
                    half_copy(c, h).wait_recv()

            @pl.when(me == 0)
            def _():
                sum_copy(1, me, c).wait_recv()

            out_ref[:, cols(c)] = (
                x_ref[:, cols(c)].astype(jnp.float32)
                + parts[me, :, cols(c)].astype(jnp.float32)
                + incoming[me + way, :, cols(c)].astype(jnp.float32)
            ).astype(out_ref.dtype)

        each(0, PIECES, finish)

    @pl.when(jnp.logical_not(is_end))
    def _():
        last = jnp.where(is_lower, n - 1, 1)
        last_way = jnp.where(is_lower, 1, 0)
        up_lag = jnp.where(is_lower, 0, 3)
        down_lag = jnp.where(is_lower, 2, 0)
        lag = up_lag + down_lag
        split = jnp.where(is_lower, n - 1, 1)
        share = PIECES // SLOT
        follows = jnp.logical_not(leads)

        def attend(i):
            attend_block(i)

        def multiply_three(c):
            multiply_piece(0, 3, cols(c))

        @pl.when(leads)
        def _():
            def both(c):
                @pl.when(jnp.logical_and(c >= up_lag, c < PIECES + up_lag))
                def _():
                    forward(0, 0, c - up_lag)

                @pl.when(jnp.logical_and(c >= down_lag, c < PIECES + down_lag))
                def _():
                    forward(1, me + 1, c - down_lag)

                @pl.when(jnp.logical_and(c == PIECES, is_lower))
                def _():
                    rest_of_own()

                @pl.when(c == lag)
                def _():
                    wait_inputs()

                @pl.when(c >= lag)
                def _():
                    multiply_three(c - lag)

            each(0, PIECES + lag, both)

            pl.when(me > 1)(give_turn)


        @pl.when(follows)
        def _():
            wait_inputs()
            way = jnp.where(is_lower, 0, 1)
            first = jnp.where(is_lower, 0, n - 1)
            second = jnp.where(is_lower, 2, 0)
            take_turn()
            pl.when(me > 1)(send_own)
            each(0, PIECES, lambda c: forward(way, first, c))
            pl.when(is_lower)(rest_of_own)
            take_turn()
            pl.when(is_lower)(send_own)

            def then(c):
                forward(1 - way, second, c)
                multiply_three(c)

            each(0, PIECES, then)

        wait_tables()

        @pl.when(is_lower)
        def _():
            def attend_forward(i):
                attend(i)
                each(i * share, (i + 1) * share, lambda c: forward(1, n - 1, c))
                pl.when(jnp.logical_and(i == 1, leads))(give_turn)

            each(0, n - 1, attend_forward)
            pl.when(follows)(give_turn)


            def out_piece(c):
                project(0, 3, cols(c))

                @pl.when(c < PIECES - (n - 1) * share)
                def _():
                    forward(1, n - 1, c + (n - 1) * share)

                pl.when(jnp.logical_and(c == TURN, leads))(give_turn)

            each(0, PIECES, out_piece)


        @pl.when(jnp.logical_not(is_lower))
        def _():
            each(0, PIECES // 2, lambda c: forward(0, 1, c))
            attend(0)

            def out_piece(c):
                @pl.when(c < PIECES // 2)
                def _():
                    forward(0, 1, c + PIECES // 2)

                project(0, 1, cols(c))

            each(0, PIECES, out_piece)
            rest_of_own()
            pl.when(leads)(give_turn)

        def multiply_last(c):
            multiply_piece(3, 1, cols(c))

        each(0, PIECES, multiply_last)
        each(split, n, attend)


        @pl.when(is_lower)
        def _():
            each(0, PIECES, lambda c: project(n - 1, 1, cols(c)))

            def stream(k):
                @pl.when(k < PIECES)
                def _():
                    pass_on(2, k)

                @pl.when(k >= PIECES)
                def _():
                    pass_last(k - PIECES)

                @pl.when(jnp.logical_and(k >= LAG, k < PIECES + LAG))
                def _():
                    pass_on(0, k - LAG)

            @pl.when(leads)
            def _():
                take_turn()
                each(0, PIECES, lambda c: pass_on(2, c))
                each(0, PIECES, pass_last)
                take_turn()
                each(0, PIECES, lambda c: pass_on(0, c))

            @pl.when(follows)
            def _():
                give_turn()
                each(0, 2 * PIECES, stream)

        @pl.when(jnp.logical_not(is_lower))
        def _():
            def out_piece(c):
                project(1, 3, cols(c))
                pass_on(0, c)
                pl.when(jnp.logical_and(c == 1, follows))(give_turn)

            each(0, PIECES, out_piece)

            def two(c):
                @pl.when(c < PIECES)
                def _():
                    pass_on(1, c)

                @pl.when(c >= LAG)
                def _():
                    pass_last(c - LAG)

            @pl.when(leads)
            def _():
                each(0, PIECES, lambda c: pass_on(1, c))
                take_turn()
                each(0, PIECES, pass_last)

            @pl.when(follows)
            def _():
                each(0, PIECES + LAG, two)

        drain_gather()

        def finish(c):
            for way in range(2):
                sum_copy(way, me, c).wait_recv()
            out_ref[:, cols(c)] = (
                x_ref[:, cols(c)].astype(jnp.float32)
                + parts[me, :, cols(c)].astype(jnp.float32)
                + incoming[me + 1, :, cols(c)].astype(jnp.float32)
                + incoming[me, :, cols(c)].astype(jnp.float32)
            ).astype(out_ref.dtype)

        each(0, PIECES, finish)

    def drain(token):
        @pl.when(token != me)
        def _():
            whole_copy(parts, rs_send.at[token], token).wait_send()

    each(0, n, drain)


def fused(layer_input, norm_gain, query_weight, key_weight, value_matrix, output_weight, keep_bits):
    n = lax.axis_size("tensor")
    rows, width = layer_input.shape
    length = n * rows
    half = HEAD_SIZE // 2
    freqs = theta_base ** (-(np.arange(half, dtype=np.float64) * 2.0) / HEAD_SIZE)
    angles = np.arange(length)[:, None] * freqs[None, :]
    cosine = np.concatenate([np.cos(angles), np.cos(angles)], axis=1).astype(np.float32)
    sine = np.concatenate([-np.sin(angles), np.sin(angles)], axis=1).astype(np.float32)
    heads = query_weight.shape[1] // HEAD_SIZE
    kv_heads = key_weight.shape[1] // HEAD_SIZE
    vmem = pl.BlockSpec(memory_space=pltpu.VMEM)
    hbm = pl.BlockSpec(memory_space=pltpu.HBM)
    bf16 = jnp.bfloat16
    weights = (query_weight, key_weight, value_matrix, output_weight)
    return pl.pallas_call(
        functools.partial(chain_kernel, n),
        out_shape=pltpu.VMEM((rows, width), bf16),
        in_specs=[hbm] * 9,
        out_specs=vmem,
        scratch_shapes=[
            pltpu.VMEM((rows, width), bf16),
            pltpu.VMEM((1, width), jnp.float32),
            pltpu.SMEM(keep_bits.shape[1:] + keep_bits.shape[:1], jnp.int32),
            pltpu.VMEM(cosine.shape, jnp.float32),
            pltpu.VMEM(sine.shape, jnp.float32),
        ]
        + [pltpu.VMEM(w.shape, bf16) for w in weights]
        + [
            pltpu.VMEM((n, rows, width), bf16),
            pltpu.VMEM((n, rows, width), bf16),
            pltpu.VMEM((n + 1, rows, width), bf16),
            pltpu.VMEM((kv_heads, length, HEAD_SIZE), bf16),
            pltpu.VMEM((kv_heads, length, HEAD_SIZE), bf16),
            pltpu.VMEM((kv_heads, heads // kv_heads * rows, HEAD_SIZE), bf16),
            pltpu.VMEM((n, rows, heads * HEAD_SIZE), bf16),
            pltpu.VMEM((n, rows, (heads + 2 * kv_heads) * HEAD_SIZE), jnp.float32),
            pltpu.SemaphoreType.DMA((9,)),
            pltpu.SemaphoreType.DMA((n + 1,)),
            pltpu.SemaphoreType.DMA((n - 1, PIECES)),
            pltpu.SemaphoreType.DMA((n,)),
            pltpu.SemaphoreType.DMA((n + HALVES, PIECES)),
            pltpu.SemaphoreType.REGULAR,
        ],
        compiler_params=pltpu.CompilerParams(
            collective_id=0, has_side_effects=True, vmem_limit_bytes=60 * 2**20
        ),
    )(layer_input, norm_gain[None, :], keep_bits.transpose(1, 2, 0), cosine, sine, *weights)


def solution(mesh):
    in_specs = (
        P(("dp", "tensor"), None),
        P(),
        P(None, "tensor"),
        P(None, "tensor"),
        P(None, "tensor"),
        P("tensor", None),
        P(("dp", "tensor"), None, None),
    )
    out_specs = P(("dp", "tensor"), None)
    return jax.shard_map(
        on_device, mesh=mesh, in_specs=in_specs, out_specs=out_specs, check_vma=False
    )
```

```python
import functools

import jax
import jax.numpy as jnp
import numpy as np
from jax import lax
from jax.experimental import pallas as pl
from jax.experimental.pallas import tpu as pltpu
from jax.sharding import PartitionSpec as P

QUERY_HEADS = 32
KEY_VALUE_HEADS = 8
HEAD_SIZE = 128
BLOCK = 64


theta_base = 1000000.0


def as_sent(array):

    def short(part):
        return part.astype(jnp.bfloat16) if part.dtype == jnp.float32 else part

    return jax.tree.map(short, array)


def from_partner(array, axis, distance):
    return lax.ppermute(array, axis, [(i, i ^ 1 << distance) for i in range(lax.axis_size(axis))])


def apply_rotary(block, token_positions):
    half = block.shape[-1] // 2
    freqs = theta_base ** (-(jnp.arange(half, dtype=jnp.float32) * 2.0) / block.shape[-1])
    angles = token_positions[:, None] * freqs[None, :]
    cosine = jnp.cos(angles)
    sine = jnp.sin(angles)
    first = block[..., :half]
    second = block[..., half:]
    return jnp.concatenate(
        [first * cosine - second * sine, second * cosine + first * sine], axis=-1
    )


def join_pairs(mine, other, lowbit):
    ahead = jnp.concatenate([mine, other], axis=-1)
    behind = jnp.concatenate([other, mine], axis=-1)
    return jnp.where(lowbit, ahead, behind)


def attend(query, key_rows, value_rows, keep_bits):
    heads, sequence_length, width = query.shape
    count = min(8, max(1, sequence_length // 512))
    height = sequence_length // count
    divisor = jnp.sqrt(jnp.float32(HEAD_SIZE))
    results = []
    for number in range(count):
        first_row = number * height
        last_row = first_row + height
        scores = (
            jnp.einsum(
                "hqd,hkd->hqk",
                query[:, first_row:last_row],
                key_rows[:, :last_row],
                preferred_element_type=jnp.float32,
            )
            / divisor
        )
        causal = jnp.arange(last_row)[None, :] <= jnp.arange(first_row, last_row)[:, None]
        scores = jnp.where(causal[None], scores, jnp.float32(-1e30))
        highest = jnp.max(scores, axis=-1, keepdims=True)
        expo_terms = jnp.exp(scores - highest)
        weights = expo_terms / jnp.sum(expo_terms, axis=-1, keepdims=True)
        chosen_bits = keep_bits[
            :, first_row // BLOCK : last_row // BLOCK, : last_row // BLOCK
        ].astype(jnp.float32)
        keeper = jnp.broadcast_to(
            chosen_bits[:, :, None, :, None],
            (heads, height // BLOCK, BLOCK, last_row // BLOCK, BLOCK),
        ).reshape(heads, height, last_row)
        dropped = (weights * keeper / 0.9).astype(jnp.bfloat16)
        outcome = jnp.einsum(
            "hqk,hkd->hqd", dropped, value_rows[:, :last_row], preferred_element_type=jnp.float32
        )
        results.append(outcome.astype(jnp.bfloat16))
    return jnp.concatenate(results, axis=1)


def on_device(
    layer_input, norm_gain, query_weight, key_weight, value_matrix, output_weight, keep_bits
):
    devices = lax.axis_size("tensor")
    paired = lax.axis_size("dp") % 2 == 0
    if devices == CHAIN and paired and layer_input.shape[0] == BLOCK:
        return fused(
            layer_input,
            norm_gain,
            query_weight,
            key_weight,
            value_matrix,
            output_weight,
            keep_bits,
        )
    position = lax.axis_index("tensor")
    sharing = devices // KEY_VALUE_HEADS if devices > KEY_VALUE_HEADS else 1
    rounds = sharing.bit_length() - 1
    inputs = layer_input.astype(jnp.float32)
    scaled = lax.rsqrt(jnp.mean(inputs * inputs, axis=-1, keepdims=True) + 1e-05)
    normed = (inputs * scaled * norm_gain[None, :]).astype(jnp.bfloat16)
    query_cols = query_weight.shape[1]
    kv_cols = key_weight.shape[1]
    piece = lax.all_gather(normed, "tensor", axis=0, tiled=True)
    projected = jnp.concatenate(
        [
            jnp.dot(piece, query_weight, preferred_element_type=jnp.float32),
            jnp.dot(piece, key_weight, preferred_element_type=jnp.float32),
            jnp.dot(piece, value_matrix, preferred_element_type=jnp.float32),
        ],
        axis=1,
    )
    query_raw = projected[:, :query_cols]
    paired = jnp.stack(
        [projected[:, query_cols : query_cols + kv_cols], projected[:, query_cols + kv_cols :]]
    ).astype(jnp.bfloat16)
    for level in range(rounds):
        other = from_partner(as_sent(paired), "tensor", level).astype(paired.dtype)
        paired = join_pairs(paired, other, position >> level & 1 == 0)
    sequence_length = query_raw.shape[0]
    local_heads = query_cols // HEAD_SIZE
    local_kv = paired.shape[2] // HEAD_SIZE
    token_positions = jnp.arange(sequence_length).astype(jnp.float32)
    query = apply_rotary(
        query_raw.reshape(sequence_length, local_heads, HEAD_SIZE).transpose(1, 0, 2),
        token_positions,
    ).astype(jnp.bfloat16)
    key_rows = apply_rotary(
        paired[0]
        .astype(jnp.float32)
        .reshape(sequence_length, local_kv, HEAD_SIZE)
        .transpose(1, 0, 2),
        token_positions,
    ).astype(jnp.bfloat16)
    value_rows = paired[1].reshape(sequence_length, local_kv, HEAD_SIZE).transpose(1, 0, 2)
    query_group = QUERY_HEADS // KEY_VALUE_HEADS
    if local_heads >= query_group:
        key_rows = jnp.repeat(key_rows, query_group, axis=0)
        value_rows = jnp.repeat(value_rows, query_group, axis=0)
    else:
        key_rows = jnp.broadcast_to(key_rows, (local_heads, sequence_length, HEAD_SIZE))
        value_rows = jnp.broadcast_to(value_rows, (local_heads, sequence_length, HEAD_SIZE))
    heads = attend(query, key_rows, value_rows, keep_bits)
    heads_out = heads.transpose(1, 0, 2).reshape(sequence_length, query_cols)
    terms = jnp.dot(heads_out, output_weight, preferred_element_type=jnp.float32).astype(
        jnp.bfloat16
    )
    total = lax.psum_scatter(terms, "tensor", scatter_dimension=0, tiled=True).astype(jnp.float32)
    return (inputs + total).astype(jnp.bfloat16)


MESH = pl.DeviceIdType.MESH
CHAIN = 4
PIECES = 8
SLOT = 4
HALVES = 1
LAG = 4
TURN = 3


def chain_kernel(
    n,
    x_hbm,
    gain_hbm,
    keep_hbm,
    cos_hbm,
    sin_hbm,
    wq_hbm,
    wk_hbm,
    wv_hbm,
    wo_hbm,
    out_ref,
    x_ref,
    gain_ref,
    keep_ref,
    cos_ref,
    sin_ref,
    wq,
    wk,
    wv,
    wo,
    gathered,
    parts,
    incoming,
    keys,
    values,
    queries,
    joined,
    projected,
    load_sem,
    ag_send,
    ag_recv,
    rs_send,
    rs_recv,
    turn,
):
    me = lax.axis_index("tensor")
    rows, width = x_ref.shape
    length = n * rows
    step = width // PIECES
    heads = wq.shape[1] // HEAD_SIZE
    kv_heads = wk.shape[1] // HEAD_SIZE
    group = heads // kv_heads
    has_left = me > 0
    has_right = me < n - 1
    is_lower = me < n // 2
    is_end = jnp.logical_or(me == 0, me == n - 1)
    pair = lax.axis_index("dp")
    leads = lax.rem(pair, 2) == 1
    partner = jnp.where(leads, pair - 1, pair + 1)

    loads = [
        pltpu.make_async_copy(src, dst, load_sem.at[i])
        for i, (src, dst) in enumerate(
            (
                (x_hbm, x_ref),
                (gain_hbm, gain_ref),
                (keep_hbm, keep_ref),
                (wk_hbm, wk),
                (wv_hbm, wv),
                (wq_hbm, wq),
                (cos_hbm, cos_ref),
                (sin_hbm, sin_ref),
                (wo_hbm, wo),
            )
        )
    ]

    barrier = pltpu.get_barrier_semaphore()

    @pl.when(has_left)
    def _():
        pl.semaphore_signal(barrier, inc=1, device_id={"tensor": me - 1}, device_id_type=MESH)

    @pl.when(has_right)
    def _():
        pl.semaphore_signal(barrier, inc=1, device_id={"tensor": me + 1}, device_id_type=MESH)

    pl.semaphore_signal(barrier, inc=1, device_id={"dp": partner}, device_id_type=MESH)

    for load in loads[:3]:
        load.start()
    loads[0].wait()
    loads[1].wait()
    for load in loads[3:]:
        load.start()

    def slot(device, block):
        return lax.rem(block + jnp.where(device == 2, 2, 0), n)

    inputs = x_ref[...].astype(jnp.float32)
    scaled = lax.rsqrt(jnp.mean(inputs * inputs, axis=-1, keepdims=True) + 1e-05)
    gathered[slot(me, me)] = (inputs * scaled * gain_ref[...]).astype(jnp.bfloat16)

    pl.semaphore_wait(barrier, jnp.where(is_end, 2, 3))

    def cols(c):
        return pl.ds(pl.multiple_of(c * step, step), step)

    def pairs(k):
        return pl.ds(pl.multiple_of(k * 2 * step, 2 * step), 2 * step)

    def other(device, block):
        return jnp.where(block > device, block - 1, block)

    def gather_copy(way, block, c):
        to = me + 1 - 2 * way
        return pltpu.make_async_remote_copy(
            src_ref=gathered.at[slot(me, block), :, cols(c)],
            dst_ref=gathered.at[slot(to, block), :, cols(c)],
            send_sem=ag_send.at[block + way],
            recv_sem=ag_recv.at[other(to, block), c],
            device_id={"tensor": to},
            device_id_type=MESH,
        )

    def arrived(block, c):
        arrival(block, c)

    def arrival(block, c):
        piece = gathered.at[slot(me, block), :, cols(c)]
        pltpu.make_async_remote_copy(
            src_ref=piece,
            dst_ref=piece,
            send_sem=ag_send.at[0],
            recv_sem=ag_recv.at[other(me, block), c],
            device_id={"tensor": jnp.where(has_right, me + 1, me - 1)},
            device_id_type=MESH,
        ).wait_recv()

    def sum_copy(way, token, c):
        return pltpu.make_async_remote_copy(
            src_ref=parts.at[token, :, cols(c)],
            dst_ref=incoming.at[token + 1 - way, :, cols(c)],
            send_sem=rs_send.at[token],
            recv_sem=rs_recv.at[token + 1 - way, c],
            device_id={"tensor": me + 1 - 2 * way},
            device_id_type=MESH,
        )

    def half_cols(c, h):
        size = step // HALVES
        return pl.ds(pl.multiple_of(c * step + h * size, size), size)

    def half_copy(c, h):
        return pltpu.make_async_remote_copy(
            src_ref=parts.at[n - 1, :, half_cols(c, h)],
            dst_ref=incoming.at[n, :, half_cols(c, h)],
            send_sem=rs_send.at[n - 1],
            recv_sem=rs_recv.at[n + h, c],
            device_id={"tensor": jnp.where(has_right, me + 1, me - 1)},
            device_id_type=MESH,
        )

    def whole_copy(buffer, sem, index):
        return pltpu.make_async_remote_copy(
            src_ref=buffer.at[index],
            dst_ref=buffer.at[index],
            send_sem=sem,
            recv_sem=ag_recv.at[0, 0],
            device_id={"tensor": jnp.where(has_right, me + 1, me - 1)},
            device_id_type=MESH,
        )

    def each(first, last, body):
        lax.fori_loop(first, last, lambda c, carry: (body(c), carry)[1], 0)

    early = jnp.where(me == 0, PIECES, jnp.where(leads, me * PIECES // 4, 0))

    def send_own():
        @pl.when(has_right)
        def _():
            each(0, early, lambda c: gather_copy(0, me, c).start())

        @pl.when(has_left)
        def _():
            each(0, PIECES, lambda c: gather_copy(1, me, c).start())

    pl.when(leads)(send_own)

    def take_turn():
        pl.semaphore_wait(turn, 1)

    def give_turn():
        pl.semaphore_signal(turn, inc=1, device_id={"dp": partner}, device_id_type=MESH)

    def rest_of_own():
        each(early, PIECES, lambda c: gather_copy(0, me, c).start())

    def forward(way, block, c):
        arrived(block, c)
        gather_copy(way, block, c).start()

    def rotated(t, cosine, sine):
        return t * cosine + pltpu.roll(t, HEAD_SIZE // 2, 1) * sine

    def multiply(first, count, where):
        block = gathered[pl.ds(first, count), :, where].reshape(count * rows, -1)
        spans = []
        at = 0
        for weight in (wq, wk, wv):
            product = jnp.dot(block, weight[where, :], preferred_element_type=jnp.float32)
            spans.append((slice(at, at + weight.shape[1]), product.reshape(count, rows, -1)))
            at += weight.shape[1]
        return spans

    def multiply_whole(first, between):
        block = gathered[first]
        at = 0
        for weight in (wq, wk, wv):
            span = slice(at, at + weight.shape[1])
            projected[first, :, span] = jnp.dot(
                block, weight[...], preferred_element_type=jnp.float32
            )
            if at == 0:
                between()
            at += weight.shape[1]

    def multiply_piece(first, count, where):
        for span, product in multiply(first, count, where):
            projected[pl.ds(first, count), :, span] += product

    def attend_block(token, length=length):
        here = slot(me, token)
        first_row = pl.multiple_of(token * rows, rows)
        where = pl.ds(first_row, rows)
        q_cols, kv_cols = wq.shape[1], wk.shape[1]
        cosine = cos_ref[where, :]
        sine = sin_ref[where, :]
        key_raw = (
            projected[here, :, q_cols : q_cols + kv_cols].astype(jnp.bfloat16).astype(jnp.float32)
        )
        value = projected[here, :, q_cols + kv_cols :].astype(jnp.bfloat16)
        for g in range(kv_heads):
            span = slice(g * HEAD_SIZE, (g + 1) * HEAD_SIZE)
            keys[g, where, :] = rotated(key_raw[:, span], cosine, sine).astype(jnp.bfloat16)
            values[g, where, :] = value[:, span]
        for g in range(kv_heads):
            wide = slice(g * group * HEAD_SIZE, (g + 1) * group * HEAD_SIZE)
            raw = projected[here, :, wide]
            for h in range(group):
                one = raw[:, h * HEAD_SIZE : (h + 1) * HEAD_SIZE]
                queries[g, h * rows : (h + 1) * rows, :] = rotated(one, cosine, sine).astype(
                    jnp.bfloat16
                )
        column = lax.broadcasted_iota(jnp.int32, (rows, length), 1)
        row = lax.broadcasted_iota(jnp.int32, (rows, length), 0) + first_row
        causal = column <= row
        which = lax.broadcasted_iota(jnp.int32, (1, length), 1) // BLOCK
        for g in range(kv_heads):
            scores = lax.dot_general(
                queries[g], keys[g, :length], (((1,), (1,)), ((), ())), preferred_element_type=jnp.float32
            ) * np.float32(1.0 / np.sqrt(HEAD_SIZE))
            dropped = []
            for h in range(group):
                one = jnp.where(causal, scores[h * rows : (h + 1) * rows], jnp.float32(-1e30))
                highest = jnp.max(one, axis=-1, keepdims=True)
                terms = jnp.exp(one - highest)
                inverse = 1.0 / (jnp.sum(terms, axis=-1, keepdims=True) * jnp.float32(0.9))
                keeper = jnp.zeros((1, length), jnp.float32)
                for j in range(length // BLOCK):
                    bit = keep_ref[token, j, g * group + h].astype(jnp.float32)
                    keeper = jnp.where(which == j, bit, keeper)
                dropped.append((terms * inverse * keeper).astype(jnp.bfloat16))
            result = jnp.dot(
                jnp.concatenate(dropped, axis=0), values[g, :length], preferred_element_type=jnp.float32
            ).astype(jnp.bfloat16)
            for h in range(group):
                at = (g * group + h) * HEAD_SIZE
                joined[token, :, at : at + HEAD_SIZE] = result[h * rows : (h + 1) * rows]

    def project(first, count, where):
        mixed = joined[pl.ds(first, count)].reshape(count * rows, -1)
        parts[pl.ds(first, count), :, where] = (
            jnp.dot(mixed, wo[:, where], preferred_element_type=jnp.float32)
            .astype(jnp.bfloat16)
            .reshape(count, rows, -1)
        )

    def pass_on(token, c):
        way = jnp.where(me < token, 0, 1)
        sum_copy(way, token, c).wait_recv()
        total = parts[token, :, cols(c)].astype(jnp.float32) + incoming[
            token + 1 - way, :, cols(c)
        ].astype(jnp.float32)
        parts[token, :, cols(c)] = total.astype(jnp.bfloat16)
        sum_copy(way, token, c).start()

    keys[...] = jnp.zeros_like(keys)
    values[...] = jnp.zeros_like(values)
    projected[...] = jnp.zeros_like(projected)
    def pass_last(c):
        for h in range(HALVES):
            where = half_cols(c, h)
            half_copy(c, h).wait_recv()
            total = parts[n - 1, :, where].astype(jnp.float32) + incoming[n, :, where].astype(
                jnp.float32
            )
            parts[n - 1, :, where] = total.astype(jnp.bfloat16)
            half_copy(c, h).start()

    def wait_inputs():
        for load in loads[3:6]:
            load.wait()


    def wait_tables():
        for load in loads[6:] + loads[2:3]:
            load.wait()

    def drain_gather():
        def drain(block):
            @pl.when(jnp.logical_and(block <= me, has_right))
            def _():
                sent(0, block)

            @pl.when(jnp.logical_and(block >= me, has_left))
            def _():
                sent(1, block)

        each(0, n, drain)

    def sent(way, block):
        whole_copy(gathered, ag_send.at[block + way], block).wait_send()

    @pl.when(is_end)
    def _():
        way = jnp.where(me == 0, 0, 1)
        wait_inputs()

        @pl.when(jnp.logical_not(leads))
        def _():
            take_turn()
            send_own()

        multiply_whole(me, lambda: pl.when(leads)(give_turn))
        wait_tables()


        def stream(i):
            def piece(k):
                arrived(i, 2 * k)
                arrived(i, 2 * k + 1)
                multiply_piece(i, 1, pairs(k))

            each(0, PIECES // 2, piece)

        def iteration(i, carry):
            @pl.when(i != me)
            def _():
                stream(i)

            @pl.when(i == 0)
            def _():
                attend_block(0, rows)

            @pl.when(i > 0)
            def _():
                attend_block(i)

            def out_piece(k):
                project(i, 1, pairs(k))
                longest = jnp.logical_and(me == 0, i == n - 1)

                @pl.when(longest)
                def _():
                    for c in (2 * k, 2 * k + 1):
                        for h in range(HALVES):
                            half_copy(c, h).start()

                @pl.when(jnp.logical_not(longest))
                def _():
                    for c in (2 * k, 2 * k + 1):
                        sum_copy(way, i, c).start()

            @pl.when(i != me)
            def _():
                each(0, PIECES // 2, out_piece)

            return carry

        lax.fori_loop(0, n, iteration, 0)

        def out_own(k):
            project(me, 1, pairs(k))

        each(0, PIECES // 2, out_own)
        drain_gather()

        def finish(c):
            @pl.when(me > 0)
            def _():
                for h in range(HALVES):
                    half_copy(c, h).wait_recv()

            @pl.when(me == 0)
            def _():
                sum_copy(1, me, c).wait_recv()

            out_ref[:, cols(c)] = (
                x_ref[:, cols(c)].astype(jnp.float32)
                + parts[me, :, cols(c)].astype(jnp.float32)
                + incoming[me + way, :, cols(c)].astype(jnp.float32)
            ).astype(out_ref.dtype)

        each(0, PIECES, finish)

    @pl.when(jnp.logical_not(is_end))
    def _():
        last = jnp.where(is_lower, n - 1, 1)
        last_way = jnp.where(is_lower, 1, 0)
        up_lag = jnp.where(is_lower, 0, 3)
        down_lag = jnp.where(is_lower, 2, 0)
        lag = up_lag + down_lag
        split = jnp.where(is_lower, n - 1, 1)
        share = PIECES // SLOT
        follows = jnp.logical_not(leads)

        def attend(i):
            attend_block(i)

        def multiply_three(c):
            multiply_piece(0, 3, cols(c))

        @pl.when(leads)
        def _():
            def both(c):
                @pl.when(jnp.logical_and(c >= up_lag, c < PIECES + up_lag))
                def _():
                    forward(0, 0, c - up_lag)

                @pl.when(jnp.logical_and(c >= down_lag, c < PIECES + down_lag))
                def _():
                    forward(1, me + 1, c - down_lag)

                @pl.when(jnp.logical_and(c == PIECES, is_lower))
                def _():
                    rest_of_own()

                @pl.when(c == lag)
                def _():
                    wait_inputs()

                @pl.when(c >= lag)
                def _():
                    multiply_three(c - lag)

            each(0, PIECES + lag, both)

            pl.when(me > 1)(give_turn)


        @pl.when(follows)
        def _():
            wait_inputs()
            way = jnp.where(is_lower, 0, 1)
            first = jnp.where(is_lower, 0, n - 1)
            second = jnp.where(is_lower, 2, 0)
            take_turn()
            pl.when(me > 1)(send_own)
            each(0, PIECES, lambda c: forward(way, first, c))
            pl.when(is_lower)(rest_of_own)
            take_turn()
            pl.when(is_lower)(send_own)

            def then(c):
                forward(1 - way, second, c)
                multiply_three(c)

            each(0, PIECES, then)

        wait_tables()

        @pl.when(is_lower)
        def _():
            def attend_forward(i):
                attend(i)
                each(i * share, (i + 1) * share, lambda c: forward(1, n - 1, c))
                pl.when(jnp.logical_and(i == 0, leads))(give_turn)

            each(0, n - 1, attend_forward)
            pl.when(follows)(give_turn)


            def out_piece(c):
                project(0, 3, cols(c))

                @pl.when(c < PIECES - (n - 1) * share)
                def _():
                    forward(1, n - 1, c + (n - 1) * share)

                pl.when(jnp.logical_and(c == TURN, leads))(give_turn)

            each(0, PIECES, out_piece)


        @pl.when(jnp.logical_not(is_lower))
        def _():
            each(0, PIECES // 2, lambda c: forward(0, 1, c))
            attend(0)

            def out_piece(c):
                @pl.when(c < PIECES // 2)
                def _():
                    forward(0, 1, c + PIECES // 2)

                project(0, 1, cols(c))

            each(0, PIECES, out_piece)
            rest_of_own()
            pl.when(leads)(give_turn)

        def multiply_last(c):
            multiply_piece(3, 1, cols(c))

        each(0, PIECES, multiply_last)
        each(split, n, attend)


        @pl.when(is_lower)
        def _():
            each(0, PIECES, lambda c: project(n - 1, 1, cols(c)))

            def stream(k):
                @pl.when(k < PIECES)
                def _():
                    pass_on(2, k)

                @pl.when(k >= PIECES)
                def _():
                    pass_last(k - PIECES)

                @pl.when(jnp.logical_and(k >= LAG, k < PIECES + LAG))
                def _():
                    pass_on(0, k - LAG)

            @pl.when(leads)
            def _():
                take_turn()
                each(0, PIECES, lambda c: pass_on(2, c))
                each(0, PIECES, pass_last)
                take_turn()
                each(0, PIECES, lambda c: pass_on(0, c))

            @pl.when(follows)
            def _():
                give_turn()
                each(0, 2 * PIECES, stream)

        @pl.when(jnp.logical_not(is_lower))
        def _():
            def out_piece(c):
                project(1, 3, cols(c))
                pass_on(0, c)
                pl.when(jnp.logical_and(c == 1, follows))(give_turn)

            each(0, PIECES, out_piece)

            def two(c):
                @pl.when(c < PIECES)
                def _():
                    pass_on(1, c)

                @pl.when(c >= LAG)
                def _():
                    pass_last(c - LAG)

            @pl.when(leads)
            def _():
                each(0, PIECES, lambda c: pass_on(1, c))
                take_turn()
                each(0, PIECES, pass_last)

            @pl.when(follows)
            def _():
                each(0, PIECES + LAG, two)

        drain_gather()

        def finish(c):
            for way in range(2):
                sum_copy(way, me, c).wait_recv()
            out_ref[:, cols(c)] = (
                x_ref[:, cols(c)].astype(jnp.float32)
                + parts[me, :, cols(c)].astype(jnp.float32)
                + incoming[me + 1, :, cols(c)].astype(jnp.float32)
                + incoming[me, :, cols(c)].astype(jnp.float32)
            ).astype(out_ref.dtype)

        each(0, PIECES, finish)

    def drain(token):
        @pl.when(token != me)
        def _():
            whole_copy(parts, rs_send.at[token], token).wait_send()

    each(0, n, drain)


def fused(layer_input, norm_gain, query_weight, key_weight, value_matrix, output_weight, keep_bits):
    n = lax.axis_size("tensor")
    rows, width = layer_input.shape
    length = n * rows
    half = HEAD_SIZE // 2
    freqs = theta_base ** (-(np.arange(half, dtype=np.float64) * 2.0) / HEAD_SIZE)
    angles = np.arange(length)[:, None] * freqs[None, :]
    cosine = np.concatenate([np.cos(angles), np.cos(angles)], axis=1).astype(np.float32)
    sine = np.concatenate([-np.sin(angles), np.sin(angles)], axis=1).astype(np.float32)
    heads = query_weight.shape[1] // HEAD_SIZE
    kv_heads = key_weight.shape[1] // HEAD_SIZE
    vmem = pl.BlockSpec(memory_space=pltpu.VMEM)
    hbm = pl.BlockSpec(memory_space=pltpu.HBM)
    bf16 = jnp.bfloat16
    weights = (query_weight, key_weight, value_matrix, output_weight)
    return pl.pallas_call(
        functools.partial(chain_kernel, n),
        out_shape=pltpu.VMEM((rows, width), bf16),
        in_specs=[hbm] * 9,
        out_specs=vmem,
        scratch_shapes=[
            pltpu.VMEM((rows, width), bf16),
            pltpu.VMEM((1, width), jnp.float32),
            pltpu.SMEM(keep_bits.shape[1:] + keep_bits.shape[:1], jnp.int32),
            pltpu.VMEM(cosine.shape, jnp.float32),
            pltpu.VMEM(sine.shape, jnp.float32),
        ]
        + [pltpu.VMEM(w.shape, bf16) for w in weights]
        + [
            pltpu.VMEM((n, rows, width), bf16),
            pltpu.VMEM((n, rows, width), bf16),
            pltpu.VMEM((n + 1, rows, width), bf16),
            pltpu.VMEM((kv_heads, length, HEAD_SIZE), bf16),
            pltpu.VMEM((kv_heads, length, HEAD_SIZE), bf16),
            pltpu.VMEM((kv_heads, heads // kv_heads * rows, HEAD_SIZE), bf16),
            pltpu.VMEM((n, rows, heads * HEAD_SIZE), bf16),
            pltpu.VMEM((n, rows, (heads + 2 * kv_heads) * HEAD_SIZE), jnp.float32),
            pltpu.SemaphoreType.DMA((9,)),
            pltpu.SemaphoreType.DMA((n + 1,)),
            pltpu.SemaphoreType.DMA((n - 1, PIECES)),
            pltpu.SemaphoreType.DMA((n,)),
            pltpu.SemaphoreType.DMA((n + HALVES, PIECES)),
            pltpu.SemaphoreType.REGULAR,
        ],
        compiler_params=pltpu.CompilerParams(
            collective_id=0, has_side_effects=True, vmem_limit_bytes=60 * 2**20
        ),
    )(layer_input, norm_gain[None, :], keep_bits.transpose(1, 2, 0), cosine, sine, *weights)


def solution(mesh):
    in_specs = (
        P(("dp", "tensor"), None),
        P(),
        P(None, "tensor"),
        P(None, "tensor"),
        P(None, "tensor"),
        P("tensor", None),
        P(("dp", "tensor"), None, None),
    )
    out_specs = P(("dp", "tensor"), None)
    return jax.shard_map(
        on_device, mesh=mesh, in_specs=in_specs, out_specs=out_specs, check_vma=False
    )
```
